128 devices in a mesh: swath: 32 (over x, y, core), chan: 4 (over z).
Axes of the slice: x: 4, y: 4, z: 4, core: 2. Of those that a mesh axis runs over, the one named last changes fastest.
Arguments:
- innovations: float32 [2097152], P(('swath', 'chan')), may hold values from -6 to 6
- obs_precision: float32 [2097152], P(('swath', 'chan')), may hold values from 0.25 to 4
- jacobian: bfloat16 [2097152, 128], P(('swath', 'chan')), may hold values from -0.5 to 0.5
- predictors: float32 [8, 2097152], P(None, ('swath', 'chan')), may hold values from -5 to 5
- obs_column: int32 [2097152], P(('swath', 'chan')), may hold values from 0 to 2047, as said below
- obs_channel: int32 [2097152], P(('swath', 'chan')), may hold values from 0 to 5119
- obs_count: int32 [32, 4], P('swath', 'chan'), may hold values from 5461 to 16384, as said below
- smoothing: float32 [128], replicated, may hold values from 0.02 to 0.12
- bias_precision: float32 [8, 5120], P(None, 'chan'), may hold values from 1 to 100
Outputs:
- control_state: float32 [1024, 256, 128], P('swath', 'chan')
- bias_increment: float32 [8, 5120], P(None, 'chan')
- residual_norms: float32 [3], replicated
The draws below stay inside these ranges and needn't reach their ends.
Inputs may be any that keep to these rules, and one draw needn't show every extreme that they name: `obs_column`: Row-major index latitude row * 64 + longitude column within the tile of the device that holds the slot; all slots of an aligned block of 128 slots lie in one latitude row. `obs_channel`: channel c belongs to block c // 256, whose coefficients are owned by chan index c // 1280. `obs_count`: slots below the count hold live observations, the rest are ignored; some device is full in every draw.
All inputs are finite; a program needn't handle non-finite values.
Results may differ from the reference program's by a relative error of at most 0.0003.
Values sent between devices are 32-bit elements; how exact they have to be, the bound alone decides.
A program may use at most 128 MiB of HBM per device.

```python
import math
import jax
import jax.numpy as jnp
from jax import lax

LEV = 128
NPRED = 8
OBS_BLOCK = 128
LAT_DEV = 32
LON_DEV = 64
OBS_DEV = 16384
ITERS = 2
OBS_ALL = 2097152
CHANNELS = 5120
N_SWATH = 32
N_CHAN = 4


def draw_obs_count(key, part):
    devices_all = N_SWATH * N_CHAN
    counts = jax.random.randint(jax.random.fold_in(key, 11), (devices_all,), OBS_DEV // 3, OBS_DEV + 1)
    fullest = jax.random.randint(jax.random.fold_in(key, 12), (), 0, devices_all)
    counts = jnp.where(jnp.arange(devices_all) == fullest, OBS_DEV, counts)
    return counts.reshape(N_SWATH, N_CHAN).astype(jnp.int32)


def draw_obs_column(key, part):
    block_count = OBS_DEV * N_SWATH * N_CHAN // OBS_BLOCK
    line_rows = jax.random.randint(jax.random.fold_in(key, 21), (block_count,), 0, LAT_DEV)
    line_cols = jax.random.randint(jax.random.fold_in(key, 22), (block_count, OBS_BLOCK), 0, LON_DEV)
    return (line_rows[:, None] * LON_DEV + line_cols).reshape(-1).astype(jnp.int32)


def touch_ends(entries, rng, smallest, largest):
    longest = entries.shape.index(max(entries.shape))
    spots = []
    for shift in (0, 1):
        where = [jax.random.randint(jax.random.fold_in(rng, axis), (), 0, length) for axis, length in enumerate(entries.shape)]
        where[longest] = (where[longest] + shift) % entries.shape[longest]
        spots.append(tuple(where))
    return entries.at[spots[0]].set(smallest).at[spots[1]].set(largest)


def steps_of(own_key, dims, split, least, top_value):
    def one(axis_at, blocks):
        draws = jax.random.uniform(jax.random.fold_in(jax.random.fold_in(own_key, 6), axis_at), (blocks,), jnp.float32, least / len(split), top_value / len(split))
        return jnp.repeat(jnp.exp(draws), dims[axis_at] // blocks).reshape((-1,) + (1,) * (len(dims) - axis_at - 1))

    level = one(*split[0])
    for cut in split[1:]:
        level = level * one(*cut)
    return level


def centred(own_key, shape, deviation, most, pieces=(), kind=jnp.bfloat16):
    result = jax.random.normal(own_key, shape, jnp.float32) * deviation
    if len(pieces) > 0:
        result = steps_of(own_key, shape, pieces, -0.22, 0.18) * result
    return jnp.clip(result, min=-most, max=most).astype(kind)


def setup_inputs(seed: int = 0) -> dict:
    arg_keys = jax.random.split(jax.random.key(seed), 10)
    innovations = centred(arg_keys[0], (OBS_ALL,), 1.0, 6.0, ((0, 128),), jnp.float32)
    obs_precision = jnp.clip(jnp.exp(math.log(4.0) - 2.7725887 * jax.random.uniform(arg_keys[1], (OBS_ALL,), jnp.float32) ** steps_of(arg_keys[1], (OBS_ALL,), ((0, 128),), -0.2, 0.2)), 0.25, 4.0)
    jacobian = centred(arg_keys[2], (OBS_ALL, LEV), LEV ** -0.5, 0.5, ((0, 128),))
    predictors = centred(arg_keys[3], (NPRED, OBS_ALL), 1.0, 5.0, ((1, 128),), jnp.float32)
    obs_column = draw_obs_column(jax.random.fold_in(arg_keys[9], 71), 0)
    obs_channel = touch_ends(jax.random.randint(arg_keys[5], (OBS_ALL,), 0, CHANNELS), jax.random.fold_in(arg_keys[5], 1), 0, CHANNELS - 1).astype(jnp.int32)
    obs_count = draw_obs_count(jax.random.fold_in(arg_keys[9], 71), 0)
    smoothing = jnp.clip(jnp.exp(jax.random.uniform(arg_keys[7], (LEV,), jnp.float32, math.log(0.02), math.log(0.12))), 0.02, 0.12)
    bias_precision = jnp.clip(jnp.exp(math.log(100.0) - 4.6051702 * jax.random.uniform(arg_keys[8], (NPRED, CHANNELS), jnp.float32) ** steps_of(arg_keys[8], (NPRED, CHANNELS), ((1, 4),), -0.2, 0.2)), 1.0, 100.0)
    return dict(innovations=innovations, obs_precision=obs_precision, jacobian=jacobian, predictors=predictors, obs_column=obs_column, obs_channel=obs_channel, obs_count=obs_count, smoothing=smoothing, bias_precision=bias_precision)


def smooth_field(state_field, smoothing):
    padded = jnp.pad(state_field, ((1, 1), (0, 0), (0, 0)))
    beside = padded[:-2] + padded[2:] + jnp.roll(state_field, 1, axis=1) + jnp.roll(state_field, -1, axis=1)
    return state_field + smoothing * (beside - 4.0 * state_field)

def reference(innovations, obs_precision, jacobian, predictors, obs_column, obs_channel, obs_count, smoothing, bias_precision):
    devices_all = N_SWATH * N_CHAN
    lat_all = LAT_DEV * N_SWATH
    lon_all = LON_DEV * N_CHAN
    cells_all = lat_all * lon_all
    slot_ids = jnp.arange(devices_all * OBS_DEV, dtype=jnp.int32)
    holder = slot_ids // OBS_DEV
    row_index = holder // N_CHAN * LAT_DEV + obs_column // LON_DEV
    col_index = holder % N_CHAN * LON_DEV + obs_column % LON_DEV
    flat_cell = (row_index * lon_all + col_index).astype(jnp.int32)
    live = slot_ids % OBS_DEV < obs_count.reshape(-1)[holder]
    weights = jnp.where(live, obs_precision, jnp.zeros_like(obs_precision))
    jac_blocks = jacobian.reshape(devices_all, OBS_DEV, LEV)
    cell_blocks = flat_cell.reshape(devices_all, OBS_DEV)

    def forward(state_field):
        table = state_field.reshape(cells_all, LEV)

        def one_block(pair):
            return lax.optimization_barrier(jnp.sum(pair[0].astype(jnp.float32) * table[pair[1]], axis=1))
        return lax.map(one_block, (jac_blocks, cell_blocks)).reshape(-1)

    def adjoint(values):
        value_blocks = values.reshape(devices_all, OBS_DEV)

        def add_block(table, triple):
            return (table.at[triple[1]].add(triple[0].astype(jnp.float32) * triple[2][:, None]), 0)
        start_table = jnp.zeros((cells_all, LEV), jnp.float32)
        table = lax.scan(add_block, start_table, (jac_blocks, cell_blocks, value_blocks))[0]
        return table.reshape(lat_all, lon_all, LEV)

    def bias_forward(coefs):
        return lax.optimization_barrier(jnp.sum(predictors * coefs[:, obs_channel], axis=0))

    def bias_adjoint(terms):
        return jnp.zeros((NPRED, CHANNELS), jnp.float32).at[:, obs_channel].add(terms)

    def hessian(state_dir, bias_dir):
        image = weights * (forward(smooth_field(state_dir, smoothing)) + bias_forward(bias_dir))
        return (state_dir + smooth_field(adjoint(image), smoothing), bias_precision * bias_dir + bias_adjoint(predictors * image[None, :]))
    source = weights * innovations
    res_state = smooth_field(adjoint(source), smoothing)
    res_bias = bias_adjoint(predictors * source[None, :])
    diagonal = bias_precision + bias_adjoint(predictors * predictors * weights[None, :])
    sol_state = jnp.zeros_like(res_state)
    sol_bias = jnp.zeros_like(res_bias)
    pre_bias = res_bias / diagonal
    dir_state, dir_bias = (res_state, pre_bias)
    state_sq = jnp.sum(res_state * res_state)
    rz_now = state_sq + jnp.sum(res_bias * pre_bias)
    record = [state_sq + jnp.sum(res_bias * res_bias)]
    for turn_index in range(ITERS):
        img_state, img_bias = hessian(dir_state, dir_bias)
        length = rz_now / (jnp.sum(dir_state * img_state) + jnp.sum(dir_bias * img_bias))
        sol_state = sol_state + length * dir_state
        sol_bias = sol_bias + length * dir_bias
        res_state = res_state - length * img_state
        res_bias = res_bias - length * img_bias
        pre_bias = res_bias / diagonal
        state_sq = jnp.sum(res_state * res_state)
        rz_next = state_sq + jnp.sum(res_bias * pre_bias)
        record.append(state_sq + jnp.sum(res_bias * res_bias))
        ratio = rz_next / rz_now
        dir_state = res_state + ratio * dir_state
        dir_bias = pre_bias + ratio * dir_bias
        rz_now = rz_next
    return (sol_state, sol_bias, jnp.sqrt(jnp.stack(record)))
```

```python
import jax
import jax.numpy as jnp
from jax import lax
from jax.experimental import pallas as pl
from jax.experimental.pallas import tpu as pltpu
from jax.sharding import Mesh
from jax.sharding import PartitionSpec as P

LEV = 128
NPRED = 8
LINES = 128
LAT = 32
LON = 64
TILES = 40
AX = ("swath_0", "swath_1", "swath_2", "chan")
SWATH = AX[:3]
MESH = pl.DeviceIdType.MESH
NT = (((1,), (1,)), ((), ()))
bf16, f32, i32 = jnp.bfloat16, jnp.float32, jnp.int32
KL = 8
UN = 8


def split(t):
    hi = t.astype(bf16)
    return hi, (t - hi.astype(f32)).astype(bf16)


def bc(row, n):
    return jnp.broadcast_to(row, (n, 128))


def lanes(b):
    return pl.ds(pl.multiple_of(b * 128, 128), 128)


def sum8(x):
    return jnp.sum(x, axis=0, keepdims=True)


def lookup(tab, ch_ref, pred_ref, out_ref):
    def step(i, _):
        for u in range(UN):
            b = i * UN + u
            ch = bc(ch_ref[pl.ds(b, 1), :], 8)
            lo, hi = ch & 127, ch >> 7
            acc = jnp.zeros((8, 128), f32)
            for h in range(TILES):
                g = jnp.take_along_axis(tab[h], lo, axis=1, mode="promise_in_bounds")
                acc = jnp.where(hi == h, g, acc)
            out_ref[pl.ds(b, 1), :] = sum8(acc * pred_ref[:, lanes(b)])
        return 0

    lax.fori_loop(0, LINES // UN, step, 0)


def forward(u2, jac, sm_i, col_ref, out_ref):
    iota = lax.broadcasted_iota(i32, (LON, 128), 0)

    def step(i, _):
        for u in range(UN):
            b = i * UN + u
            both = lax.dot_general(u2[sm_i[4, b]], jac[b], NT, preferred_element_type=f32)
            s = both[:LON] + both[LON:]
            m = iota == bc(col_ref[pl.ds(b, 1), :], LON)
            out_ref[pl.ds(b, 1), :] = sum8(jnp.where(m, s, 0.0))
        return 0

    lax.fori_loop(0, LINES // UN, step, 0)


def adjoint(y_ref, jac, sm_i, col_ref, seg):
    iota = lax.broadcasted_iota(i32, (LON, 128), 0)

    def step(i, acc):
        for u in range(UN):
            k = i * UN + u
            b = sm_i[0, k]
            y = y_ref[pl.ds(b, 1), :]
            hi = y.astype(bf16).astype(f32)
            lo = y - hi
            m = iota == bc(col_ref[pl.ds(b, 1), :], LON)
            parts = [jnp.where(m, bc(t, LON), 0.0) for t in (hi, lo)]
            a = jnp.concatenate(parts, axis=0).astype(bf16)
            both = jnp.dot(a, jac[b], preferred_element_type=f32)
            same = sm_i[1, k] == sm_i[1, jnp.maximum(k - 1, 0)]
            acc = jnp.where(same, acc, 0.0) + (both[:LON] + both[LON:])
            seg[k] = acc
        return acc

    lax.fori_loop(0, LINES // UN, step, jnp.zeros((LON, 128), f32))


def make_hot(ch_ref, oh):
    iota = lax.broadcasted_iota(i32, (256, 128), 0)

    def step(b, _):
        ch = ch_ref[pl.ds(b, 1), :] & 255
        oh[:, lanes(b)] = jnp.where(iota == bc(ch, 256), 1.0, 0.0).astype(bf16)
        return 0

    lax.fori_loop(0, LINES, step, 0)


def bias_adjoint(terms, ch_ref, oh, lhs, acc):
    rows, k = 320 * len(terms), KL * 128

    def step(c, _):
        for l in range(KL):
            b = c * KL + l
            hb = bc((ch_ref[pl.ds(b, 1), :] >> 8).astype(f32), 16).astype(bf16)
            for j, f in enumerate(terms):
                st = jnp.concatenate(split(f(b)), axis=0)
                for h in range(20):
                    at = (j * 20 + h) * 16
                    lhs[at : at + 16, l * 128 : (l + 1) * 128] = jnp.where(
                        hb == jnp.asarray(h, bf16), st, jnp.zeros((), bf16)
                    )
        part = lax.dot_general(
            lhs[:rows], oh[:, pl.ds(pl.multiple_of(c * k, k), k)], NT, preferred_element_type=f32
        )
        acc[:rows] += part
        return 0

    acc[:rows] = jnp.zeros((rows, 256), f32)
    lax.fori_loop(0, LINES // KL, step, 0)


def acc_tile(acc, j, t):
    at, ls = (j * 20 + t // 2) * 16, slice((t % 2) * 128, (t % 2) * 128 + 128)
    return acc[at : at + 8, ls] + acc[at + 8 : at + 16, ls]


def wait_all(ref, sem):
    pltpu.make_async_copy(ref, ref, sem).wait()


def kernel(
    innov, prec, jac_hbm, pred, col, chan, count, smooth, biasp,
    out_x, out_b, out_n,
    jac, oh, lhs, acc, w, y, hs, pc, u2, seg, gp, r0, r1, q0, xs, est, hcol, cn,
    rs0_send, rs0_recv, rs_send, rs_recv, zt, sca, scb, ob, iv, cl, sm_i,
    s_load, s_halo_s, s_halo_r, s_rs_s, s_rs_r, s_ag_s, s_ag_r, s_sc_s, s_sc_r,
):
    x, yy, c, z = (lax.axis_index(a) for a in AX)
    s = (x * 4 + yy) * 2 + c
    owner = (lax.rem(s, 3) == 0) & (s < 30)
    mine = z * 10 + lax.div(s, 3)
    me = s * 4 + z

    def coords(sw):
        return lax.div(sw, 8), lax.rem(lax.div(sw, 2), 4), lax.rem(sw, 2)

    load_j = pltpu.make_async_copy(jac_hbm, jac, s_load.at[0])
    load_j.start()
    for ph in range(3):
        for r in (0, 1, 34, 35):
            gp[ph, r] = jnp.zeros((80, 128), f32)

    def everyone(f):
        def step(i, _):
            tx = lax.rem(x + lax.div(i, 4), 4)
            ty = lax.rem(yy + lax.rem(i, 4), 4)
            for dc in range(2):
                for dz in range(4):
                    to = (tx, ty, lax.rem(c + dc, 2), lax.rem(z + dz, 4))
                    if dc == 0 and dz == 0:
                        pl.when(i > 0)(lambda to=to: f(to))
                    else:
                        f(to)
            return 0

        lax.fori_loop(0, 16, step, 0)

    barrier = pltpu.get_barrier_semaphore()
    everyone(lambda to: pl.semaphore_signal(barrier, inc=1, device_id=to, device_id_type=MESH))

    slot = lax.broadcasted_iota(i32, (LINES, 128), 0) * 128 + lax.broadcasted_iota(i32, (LINES, 128), 1)
    w[...] = jnp.where(slot < count[0, 0], prec[...], 0.0)
    y[...] = w[...] * innov[...]

    iota_s = lax.broadcasted_iota(i32, (128, 128), 0)
    iota_l = lax.broadcasted_iota(i32, (128, 128), 1)

    def count_of(m, v=1):
        return sum8(jnp.where(m, v, 0))

    a = jnp.broadcast_to(col[:, 0:1] >> 6, (128, 128))
    row_l = count_of(iota_s == iota_l, a)
    b = bc(row_l, 128)
    rank = jnp.transpose(bc(count_of((a < b) | ((a == b) & (iota_s < iota_l))), 128))
    put = rank == iota_l
    iv[0:1] = count_of(put, iota_s)
    iv[1:2] = count_of(put, a)
    iv[2:3] = jnp.maximum(count_of(a <= iota_l) - 1, 0)
    iv[3:4] = count_of(a == iota_l)
    iv[4:5] = row_l
    iv[5:8] = jnp.zeros((3, 128), i32)
    to_smem = pltpu.make_async_copy(iv, sm_i, s_load.at[1])
    to_smem.start()
    make_hot(chan, oh)
    cl[...] = col[...] & 63

    for i in range(8):
        ob[i] = jnp.zeros((8, 128), f32)

    def scatter(send, recv, ph):
        def step(i, _):
            tz = lax.rem(z + lax.div(i, 10), 4)
            j = lax.rem(s + lax.rem(i, 10), 10)
            t = tz * 10 + j
            to = coords(3 * j) + (tz,)

            @pl.when((3 * j != s) | (tz != z))
            def _():
                pltpu.make_async_remote_copy(
                    src_ref=send.at[t], dst_ref=recv.at[me], send_sem=s_rs_s.at[ph],
                    recv_sem=s_rs_r.at[ph], device_id=to, device_id_type=MESH,
                ).start()

            return 0

        lax.fori_loop(0, TILES, step, 0, unroll=4)

        @pl.when(owner)
        def _():
            recv[me] = send[mine]

    def gathered(recv, ph):
        wait_all(recv.at[pl.ds(0, 127)], s_rs_r.at[ph])
        total = recv[0]
        for i in range(1, 128):
            total += recv[i]
        return total

    def spread(k):
        def send(to):
            pltpu.make_async_remote_copy(
                src_ref=zt.at[k, mine], dst_ref=zt.at[k, mine], send_sem=s_ag_s.at[k],
                recv_sem=s_ag_r.at[k], device_id=to, device_id_type=MESH,
            ).start()

        everyone(send)

    def wait_spread(k):
        @pl.when(owner)
        def _():
            wait_all(zt.at[k, pl.ds(0, TILES - 1)], s_ag_r.at[k])

        @pl.when(jnp.logical_not(owner))
        def _():
            wait_all(zt.at[k], s_ag_r.at[k])

    def scalars_a(ph, rows):
        n = len(rows)
        mya = c * 4 + z
        sca[ph, mya] = jnp.concatenate(list(rows) + [jnp.zeros((8 - n, 128), f32)], axis=0)
        for d in range(1, 8):
            to = (x, yy, lax.rem(c + d // 4, 2), lax.rem(z + d % 4, 4))
            pltpu.make_async_remote_copy(
                src_ref=sca.at[ph, mya], dst_ref=sca.at[ph, mya], send_sem=s_sc_s.at[ph, 0],
                recv_sem=s_sc_r.at[ph, 0], device_id=to, device_id_type=MESH,
            ).start()

    def scalars_b(ph):
        wait_all(sca.at[ph, pl.ds(0, 7)], s_sc_r.at[ph, 0])
        total = sca[ph, 0]
        for i in range(1, 8):
            total += sca[ph, i]
        myb = x * 4 + yy
        scb[ph, myb] = total
        for d in range(1, 16):
            to = (lax.rem(x + d // 4, 4), lax.rem(yy + d % 4, 4), c, z)
            pltpu.make_async_remote_copy(
                src_ref=scb.at[ph, myb], dst_ref=scb.at[ph, myb], send_sem=s_sc_s.at[ph, 1],
                recv_sem=s_sc_r.at[ph, 1], device_id=to, device_id_type=MESH,
            ).start()

    def scalars_c(ph):
        wait_all(scb.at[ph, pl.ds(0, 15)], s_sc_r.at[ph, 1])
        total = scb[ph, 0]
        for i in range(1, 16):
            total += scb[ph, i]
        sums = jnp.sum(total, axis=1, keepdims=True)
        return sums[0:1], sums[1:2], sums[2:3]

    above, below = coords(s - 1), coords(s + 1)
    left, right = lax.rem(z + 3, 4), lax.rem(z + 1, 4)
    has_above, has_below = s > 0, s < 31

    def halo_copies(ph):
        def mk(n, src, dst, to):
            return pltpu.make_async_remote_copy(
                src_ref=src, dst_ref=dst, send_sem=s_halo_s.at[ph, n],
                recv_sem=s_halo_r.at[ph, n], device_id=to, device_id_type=MESH,
            )

        g = gp.at[ph]
        mid = pl.ds(8, LON)
        sides = [
            mk(0, est.at[ph, 0], hcol.at[ph, 1], (x, yy, c, left)),
            mk(1, est.at[ph, 1], hcol.at[ph, 0], (x, yy, c, right)),
        ]
        up = [
            mk(2, g.at[pl.ds(2, 2), mid], g.at[pl.ds(34, 2), mid], above + (z,)),
            mk(3, g.at[2, pl.ds(8, 8)], cn.at[ph, 0], above + (left,)),
            mk(4, g.at[2, pl.ds(64, 8)], cn.at[ph, 1], above + (right,)),
        ]
        down = [
            mk(5, g.at[pl.ds(32, 2), mid], g.at[pl.ds(0, 2), mid], below + (z,)),
            mk(6, g.at[33, pl.ds(8, 8)], cn.at[ph, 2], below + (left,)),
            mk(7, g.at[33, pl.ds(64, 8)], cn.at[ph, 3], below + (right,)),
        ]
        return sides, up, down

    def halo_send(ph):
        for r in range(LAT):
            g = jnp.where(sm_i[3, r] > 0, seg[sm_i[2, r]], 0.0)
            gp[ph, r + 2, 8:72, :] = g
            est[ph, 0, 2 * r : 2 * r + 2, :] = g[0:2]
            est[ph, 1, 2 * r : 2 * r + 2, :] = g[62:64]
        sides, up, down = halo_copies(ph)
        for cp in sides:
            cp.start()

        @pl.when(has_above)
        def _():
            for cp in up:
                cp.start()

        @pl.when(has_below)
        def _():
            for cp in down:
                cp.start()

    def halo_wait(ph):
        sides, up, down = halo_copies(ph)
        for cp in sides:
            cp.wait_recv()

        @pl.when(has_below)
        def _():
            for cp in up:
                cp.wait_recv()
            gp[ph, 34, 72:73, :] = cn[ph, 0, 0:1]
            gp[ph, 34, 7:8, :] = cn[ph, 1, 7:8]

        @pl.when(has_above)
        def _():
            for cp in down:
                cp.wait_recv()
            gp[ph, 1, 72:73, :] = cn[ph, 2, 0:1]
            gp[ph, 1, 7:8, :] = cn[ph, 3, 7:8]

        for r in range(LAT):
            gp[ph, r + 2, 72:74, :] = hcol[ph, 1, 2 * r : 2 * r + 2]
            gp[ph, r + 2, 6:8, :] = hcol[ph, 0, 2 * r : 2 * r + 2]

    def halo_done(ph):
        sides, up, down = halo_copies(ph)
        for cp in sides:
            cp.wait_send()

        @pl.when(has_above)
        def _():
            for cp in up:
                cp.wait_send()

        @pl.when(has_below)
        def _():
            for cp in down:
                cp.wait_send()

    sm = smooth[...]

    def smoothed(ref, r):
        v = ref[r]
        beside = ref[r - 1] + ref[r + 1] + pltpu.roll(v, 1, 0) + pltpu.roll(v, 79, 0)
        return v + sm * (beside - 4.0 * v)

    def inside(r):
        return ((r > 1) | has_above) & ((r < 34) | has_below)

    def squares(v):
        v = v * v
        t = v[0:8]
        for i in range(1, LON // 8):
            t += v[8 * i : 8 * i + 8]
        return t

    def to_forward(src):
        def step(r, total):
            u = smoothed(src, r)[8:72]
            hi, lo = split(u)
            u2[r - 2, 0:LON] = hi
            u2[r - 2, LON : 2 * LON] = lo
            return total + squares(src[r, 8:72, :])

        return sum8(lax.fori_loop(2, 34, step, jnp.zeros((8, 128), f32)))

    def slots_of(k):
        wait_spread(k)
        lookup(zt.at[k], chan, pred, pc)
        image = hs[...] + pc[...]
        yw = w[...] * image
        y[...] = yw
        return sum8(yw * image)

    def term_y(b):
        return pred[:, lanes(b)] * y[pl.ds(b, 1), :]

    def term_d(b):
        p = pred[:, lanes(b)]
        return p * p * w[pl.ds(b, 1), :]

    bias_adjoint([term_y, term_d], chan, oh, lhs, acc)
    for t in range(TILES):
        rs0_send[t, 0:8] = acc_tile(acc, 0, t)
        rs0_send[t, 8:16] = acc_tile(acc, 1, t)
    pl.semaphore_wait(barrier, 127)
    scatter(rs0_send, rs0_recv, 0)
    to_smem.wait()
    load_j.wait()
    adjoint(y, jac, sm_i, cl, seg)
    halo_send(0)

    @pl.when(owner)
    def _():
        both = gathered(rs0_recv, 0)
        bp = biasp[:, lanes(lax.div(s, 3))]
        rb, dg = both[0:8], both[8:16] + bp
        zb = rb / dg
        ob[0] = rb
        ob[1] = dg
        ob[2] = zb
        ob[3] = bp
        zt[0, mine] = zb
        spread(0)

    halo_wait(0)

    def first(r, _):
        r0[r] = jnp.where(inside(r), smoothed(gp.at[0], r), 0.0)
        return 0

    lax.fori_loop(1, 35, first, 0)
    rr_state = to_forward(r0)

    forward(u2, jac, sm_i, cl, hs)
    d0 = slots_of(0)
    scalars_a(0, (
        rr_state + sum8(ob[0] * ob[2]),
        rr_state + d0 + sum8(ob[3] * ob[2] * ob[2]),
        rr_state + sum8(ob[0] * ob[0]),
    ))
    bias_adjoint([term_y], chan, oh, lhs, acc)
    for t in range(TILES):
        rs_send[0, t] = acc_tile(acc, 0, t)
    scatter(rs_send.at[0], rs_recv.at[0], 1)
    scalars_b(0)
    adjoint(y, jac, sm_i, cl, seg)
    halo_send(1)
    rz0, pq0, rr0 = scalars_c(0)
    alpha0 = rz0 / pq0

    @pl.when(owner)
    def _():
        qb = ob[3] * ob[2] + gathered(rs_recv.at[0], 1)
        rb = ob[0] - alpha0 * qb
        zb = rb / ob[1]
        ob[4] = qb
        ob[5] = rb
        ob[6] = zb
        zt[1, mine] = zb
        spread(1)

    halo_wait(1)

    def second(r, _):
        q = r0[r] + jnp.where(inside(r), smoothed(gp.at[1], r), 0.0)
        q0[r] = q
        r1[r] = r0[r] - alpha0 * q
        return 0

    lax.fori_loop(1, 35, second, 0)
    rr_state = to_forward(r1)

    forward(u2, jac, sm_i, cl, hs)
    d1 = slots_of(1)
    scalars_a(1, (
        rr_state + sum8(ob[5] * ob[6]),
        rr_state + d1 + sum8(ob[3] * ob[6] * ob[6]),
        rr_state + sum8(ob[5] * ob[5]),
    ))
    bias_adjoint([term_y], chan, oh, lhs, acc)
    for t in range(TILES):
        rs_send[1, t] = acc_tile(acc, 0, t)
    scatter(rs_send.at[1], rs_recv.at[1], 2)
    scalars_b(1)
    adjoint(y, jac, sm_i, cl, seg)
    halo_send(2)
    rz1, zaz, rr1 = scalars_c(1)
    beta = rz1 / rz0
    alpha1 = rz1 / (zaz - beta * rz1 / alpha0)
    mix = alpha0 + alpha1 * beta

    def solved(r, _):
        xs[r - 2] = mix * r0[r, 8:72, :] + alpha1 * r1[r, 8:72, :]
        return 0

    lax.fori_loop(2, 34, solved, 0)
    store_x = pltpu.make_async_copy(xs, out_x, s_load.at[2])
    store_x.start()
    for t in range(10):
        at = z * 10 + t
        out_b[:, t * 128 : (t + 1) * 128] = mix * zt[0, at] + alpha1 * zt[1, at]

    @pl.when(owner)
    def _():
        qb = ob[3] * ob[6] + gathered(rs_recv.at[1], 2) + beta * ob[4]
        ob[7] = ob[5] - alpha1 * qb

    halo_wait(2)

    def last(r, total):
        v = r1[r, 8:72, :]
        q = v + smoothed(gp.at[2], r)[8:72] + beta * q0[r, 8:72, :]
        return total + squares(v - alpha1 * q)

    rr_state = sum8(lax.fori_loop(2, 34, last, jnp.zeros((8, 128), f32)))
    scalars_a(2, (rr_state + sum8(ob[7] * ob[7]),))
    scalars_b(2)
    rr2, _, _ = scalars_c(2)
    lane = lax.broadcasted_iota(i32, (1, 128), 1)
    out_n[...] = jnp.sqrt(jnp.where(lane == 0, rr0, jnp.where(lane == 1, rr1, rr2)))

    for ph, ref in ((0, rs0_send), (1, rs_send.at[0]), (2, rs_send.at[1])):
        @pl.when(owner)
        def _(ph=ph, ref=ref):
            wait_all(ref.at[pl.ds(0, TILES - 1)], s_rs_s.at[ph])

        @pl.when(jnp.logical_not(owner))
        def _(ph=ph, ref=ref):
            wait_all(ref, s_rs_s.at[ph])

    @pl.when(owner)
    def _():
        for k in range(2):
            wait_all(rs_recv.at[0, pl.ds(0, 127)], s_ag_s.at[k])

    for ph in range(3):
        halo_done(ph)
        wait_all(sca.at[ph, pl.ds(0, 7)], s_sc_s.at[ph, 0])
        wait_all(scb.at[ph, pl.ds(0, 15)], s_sc_s.at[ph, 1])
    store_x.wait()


def body(innovations, obs_precision, jacobian, predictors, obs_column, obs_channel, obs_count, smoothing, bias_precision):
    vm = pl.BlockSpec(memory_space=pltpu.VMEM)
    hbm = pl.BlockSpec(memory_space=pl.ANY)
    sq = (LINES, 128)
    V = pltpu.VMEM
    D = pltpu.SemaphoreType.DMA
    out = pl.pallas_call(
        kernel,
        name="pcg",
        out_shape=(
            jax.ShapeDtypeStruct((LAT, LON, LEV), f32),
            jax.ShapeDtypeStruct((NPRED, 1280), f32),
            jax.ShapeDtypeStruct((1, 128), f32),
        ),
        in_specs=[vm, vm, hbm, vm, vm, vm, pl.BlockSpec(memory_space=pltpu.SMEM), vm, vm],
        out_specs=(hbm, vm, vm),
        scratch_shapes=[
            V((LINES, 128, LEV), bf16), V((256, 16384), bf16), V((640, KL * 128), bf16), V((640, 256), f32),
            V(sq, f32), V(sq, f32), V(sq, f32), V(sq, f32),
            V((LAT, 2 * LON, LEV), bf16), V((LINES, LON, LEV), f32),
            V((3, 36, 80, LEV), f32), V((36, 80, LEV), f32), V((36, 80, LEV), f32), V((36, 80, LEV), f32),
            V((LAT, LON, LEV), f32), V((3, 2, 64, LEV), f32), V((3, 2, 64, LEV), f32), V((3, 4, 8, LEV), f32),
            V((TILES, 16, 128), f32), V((128, 16, 128), f32), V((2, TILES, 8, 128), f32), V((2, 128, 8, 128), f32),
            V((2, TILES, 8, 128), f32), V((3, 8, 8, 128), f32), V((3, 16, 8, 128), f32), V((8, 8, 128), f32),
            V((8, 128), i32), V(sq, i32), pltpu.SMEM((8, 128), i32),
            D((3,)), D((3, 8)), D((3, 8)), D((3,)), D((3,)), D((2,)), D((2,)), D((3, 2)), D((3, 2)),
        ],
        compiler_params=pltpu.CompilerParams(
            collective_id=0, has_side_effects=True, vmem_limit_bytes=62 * 2**20
        ),
    )(
        innovations.reshape(sq), obs_precision.reshape(sq), jacobian.reshape(LINES, 128, LEV), predictors,
        obs_column.reshape(sq), obs_channel.reshape(sq), obs_count, smoothing.reshape(1, LEV), bias_precision,
    )
    return out[0], out[1], out[2][0, :3]


def solution(mesh):
    torus = Mesh(mesh.devices.reshape(4, 4, 2, mesh.shape["chan"]), AX)
    placed = (
        P(AX), P(AX), P(AX, None), P(None, AX), P(AX), P(AX), P(SWATH, "chan"), P(), P(None, "chan"),
    )
    return jax.shard_map(
        body,
        mesh=torus,
        in_specs=placed,
        out_specs=(P(SWATH, "chan", None), P(None, "chan"), P()),
        check_vma=False,
    )
```

```python
import jax
import jax.numpy as jnp
from jax import lax
from jax.experimental import pallas as pl
from jax.experimental.pallas import tpu as pltpu
from jax.sharding import Mesh
from jax.sharding import PartitionSpec as P

LEV = 128
NPRED = 8
LINES = 128
LAT = 32
LON = 64
TILES = 40
AX = ("swath_0", "swath_1", "swath_2", "chan")
SWATH = AX[:3]
MESH = pl.DeviceIdType.MESH
NT = (((1,), (1,)), ((), ()))
bf16, f32, i32 = jnp.bfloat16, jnp.float32, jnp.int32
KL = 32
UN = 32


def split(t):
    hi = t.astype(bf16)
    return hi, (t - hi.astype(f32)).astype(bf16)


def bc(row, n):
    return jnp.broadcast_to(row, (n, 128))


def lanes(b):
    return pl.ds(pl.multiple_of(b * 128, 128), 128)


def sum8(x):
    return jnp.sum(x, axis=0, keepdims=True)


def make_table(zt, tab):
    for h in range(20):
        t = jnp.concatenate([zt[2 * h], zt[2 * h + 1]], axis=1)
        tab[16 * h : 16 * h + 16] = jnp.concatenate(split(t), axis=0)


def lookup(tab, oh, ch_ref, pred_ref, out_ref):
    def step(i, _):
        for g in range(UN // 2):
            b0 = i * UN + 2 * g
            hot = jnp.concatenate([oh[b0], oh[b0 + 1]], axis=1)
            got = jnp.dot(tab[...], hot, preferred_element_type=f32)
            for u in range(2):
                b, ls = b0 + u, slice(u * 128, u * 128 + 128)
                hb = bc(ch_ref[pl.ds(b, 1), :] >> 8, 8)
                hi = jnp.zeros((8, 128), f32)
                lo = hi
                for h in range(20):
                    m = hb == h
                    hi = jnp.where(m, got[16 * h : 16 * h + 8, ls], hi)
                    lo = jnp.where(m, got[16 * h + 8 : 16 * h + 16, ls], lo)
                out_ref[pl.ds(b, 1), :] = sum8((hi + lo) * pred_ref[:, lanes(b)])
        return 0

    lax.fori_loop(0, LINES // UN, step, 0)


def forward(u2, jac, sm_i, col_ref, out_ref):
    iota = lax.broadcasted_iota(i32, (LON, 128), 0)

    def step(i, _):
        for u in range(UN):
            b = i * UN + u
            both = lax.dot_general(u2[sm_i[4, b]], jac[b], NT, preferred_element_type=f32)
            s = both[:LON] + both[LON:]
            m = iota == bc(col_ref[pl.ds(b, 1), :], LON)
            out_ref[pl.ds(b, 1), :] = sum8(jnp.where(m, s, 0.0))
        return 0

    lax.fori_loop(0, LINES // UN, step, 0)


def adjoint(y_ref, jac, sm_i, col_ref, seg):
    iota = lax.broadcasted_iota(i32, (LON, 128), 0)

    def step(i, acc):
        for u in range(UN):
            k = i * UN + u
            b = sm_i[0, k]
            y = y_ref[pl.ds(b, 1), :]
            hi = y.astype(bf16).astype(f32)
            lo = y - hi
            m = iota == bc(col_ref[pl.ds(b, 1), :], LON)
            parts = [jnp.where(m, bc(t, LON), 0.0) for t in (hi, lo)]
            a = jnp.concatenate(parts, axis=0).astype(bf16)
            both = jnp.dot(a, jac[b], preferred_element_type=f32)
            same = sm_i[1, k] == sm_i[1, jnp.maximum(k - 1, 0)]
            acc = jnp.where(same, acc, 0.0) + (both[:LON] + both[LON:])
            seg[k] = acc
        return acc

    lax.fori_loop(0, LINES // UN, step, jnp.zeros((LON, 128), f32))


def make_hot(ch_ref, oh):
    iota = lax.broadcasted_iota(i32, (256, 128), 0).astype(f32).astype(bf16)
    one, zero = jnp.ones((), bf16), jnp.zeros((), bf16)

    def step(i, _):
        for u in range(8):
            b = i * 8 + u
            ch = bc((ch_ref[pl.ds(b, 1), :] & 255).astype(f32), 16).astype(bf16)
            for j in range(0, 256, 16):
                oh[b, j : j + 16] = jnp.where(iota[j : j + 16] == ch, one, zero)
        return 0

    lax.fori_loop(0, LINES // 8, step, 0)


def bias_adjoint(terms, ch_ref, oh, lhs, acc):
    n = len(terms)
    rows, kl = 320 * n, KL // n
    zero = jnp.zeros((), bf16)

    def step(c, _):
        for l in range(kl):
            b = c * kl + l
            hb = bc((ch_ref[pl.ds(b, 1), :] >> 8).astype(f32), 16).astype(bf16)
            sts = [jnp.concatenate(split(f(b)), axis=0) for f in terms]
            for h in range(20):
                m = hb == jnp.asarray(h, bf16)
                for j, st in enumerate(sts):
                    at = (j * 20 + h) * 16
                    lhs[l, at : at + 16] = jnp.where(m, st, zero)
        left = jnp.concatenate([lhs[l, :rows] for l in range(kl)], axis=1)
        hot = jnp.concatenate([oh[c * kl + l] for l in range(kl)], axis=1)
        acc[:rows] += lax.dot_general(left, hot, NT, preferred_element_type=f32)
        return 0

    acc[:rows] = jnp.zeros((rows, 256), f32)
    lax.fori_loop(0, LINES // kl, step, 0)


def acc_tile(acc, j, t):
    at, ls = (j * 20 + t // 2) * 16, slice((t % 2) * 128, (t % 2) * 128 + 128)
    return acc[at : at + 8, ls] + acc[at + 8 : at + 16, ls]


def wait_all(ref, sem):
    pltpu.make_async_copy(ref, ref, sem).wait()


def kernel(
    innov, prec, jac_hbm, pred, col, chan, count, smooth, biasp,
    out_x, out_b, out_n,
    jac, oh, lhs, acc, tab, w, y, hs, pc, u2, seg, gp, r0, r1, q0, xs, est, hcol, cn,
    rs0_send, rs0_recv, rs_send, rs_recv, zt, sca, scb, ob, iv, cl, sm_i,
    s_load, s_halo_s, s_halo_r, s_rs_s, s_rs_r, s_ag_s, s_ag_r, s_sc_s, s_sc_r,
):
    x, yy, c, z = (lax.axis_index(a) for a in AX)
    s = (x * 4 + yy) * 2 + c
    owner = (lax.rem(s, 3) == 0) & (s < 30)
    mine = z * 10 + lax.div(s, 3)
    me = s * 4 + z

    def coords(sw):
        return lax.div(sw, 8), lax.rem(lax.div(sw, 2), 4), lax.rem(sw, 2)

    load_j = pltpu.make_async_copy(jac_hbm, jac, s_load.at[0])
    load_j.start()
    for ph in range(3):
        for r in (0, 1, 34, 35):
            gp[ph, r] = jnp.zeros((80, 128), f32)

    def everyone(f):
        def step(i, _):
            tx = lax.rem(x + lax.div(i, 4), 4)
            ty = lax.rem(yy + lax.rem(i, 4), 4)
            for dc in range(2):
                for dz in range(4):
                    to = (tx, ty, lax.rem(c + dc, 2), lax.rem(z + dz, 4))
                    if dc == 0 and dz == 0:
                        pl.when(i > 0)(lambda to=to: f(to))
                    else:
                        f(to)
            return 0

        lax.fori_loop(0, 16, step, 0)

    barrier = pltpu.get_barrier_semaphore()
    everyone(lambda to: pl.semaphore_signal(barrier, inc=1, device_id=to, device_id_type=MESH))

    slot = lax.broadcasted_iota(i32, (LINES, 128), 0) * 128 + lax.broadcasted_iota(i32, (LINES, 128), 1)
    w[...] = jnp.where(slot < count[0, 0], prec[...], 0.0)
    y[...] = w[...] * innov[...]

    iota_s = lax.broadcasted_iota(i32, (128, 128), 0)
    iota_l = lax.broadcasted_iota(i32, (128, 128), 1)

    def count_of(m, v=1):
        return sum8(jnp.where(m, v, 0))

    a = jnp.broadcast_to(col[:, 0:1] >> 6, (128, 128))
    row_l = count_of(iota_s == iota_l, a)
    b = bc(row_l, 128)
    rank = jnp.transpose(bc(count_of((a < b) | ((a == b) & (iota_s < iota_l))), 128))
    put = rank == iota_l
    iv[0:1] = count_of(put, iota_s)
    iv[1:2] = count_of(put, a)
    iv[2:3] = jnp.maximum(count_of(a <= iota_l) - 1, 0)
    iv[3:4] = count_of(a == iota_l)
    iv[4:5] = row_l
    iv[5:8] = jnp.zeros((3, 128), i32)
    to_smem = pltpu.make_async_copy(iv, sm_i, s_load.at[1])
    to_smem.start()
    make_hot(chan, oh)
    cl[...] = col[...] & 63

    for i in range(8):
        ob[i] = jnp.zeros((8, 128), f32)

    def scatter(send, recv, ph):
        def step(i, _):
            tz = lax.rem(z + lax.div(i, 10), 4)
            j = lax.rem(s + lax.rem(i, 10), 10)
            t = tz * 10 + j
            to = coords(3 * j) + (tz,)

            @pl.when((3 * j != s) | (tz != z))
            def _():
                pltpu.make_async_remote_copy(
                    src_ref=send.at[t], dst_ref=recv.at[me], send_sem=s_rs_s.at[ph],
                    recv_sem=s_rs_r.at[ph], device_id=to, device_id_type=MESH,
                ).start()

            return 0

        lax.fori_loop(0, TILES, step, 0, unroll=4)

        @pl.when(owner)
        def _():
            recv[me] = send[mine]

    def gathered(recv, ph):
        wait_all(recv.at[pl.ds(0, 127)], s_rs_r.at[ph])
        total = recv[0]
        for i in range(1, 128):
            total += recv[i]
        return total

    def spread(k):
        def send(to):
            pltpu.make_async_remote_copy(
                src_ref=zt.at[k, mine], dst_ref=zt.at[k, mine], send_sem=s_ag_s.at[k],
                recv_sem=s_ag_r.at[k], device_id=to, device_id_type=MESH,
            ).start()

        everyone(send)

    def wait_spread(k):
        @pl.when(owner)
        def _():
            wait_all(zt.at[k, pl.ds(0, TILES - 1)], s_ag_r.at[k])

        @pl.when(jnp.logical_not(owner))
        def _():
            wait_all(zt.at[k], s_ag_r.at[k])

    def scalars_a(ph, rows):
        n = len(rows)
        mya = c * 4 + z
        sca[ph, mya] = jnp.concatenate(list(rows) + [jnp.zeros((8 - n, 128), f32)], axis=0)
        for d in range(1, 8):
            to = (x, yy, lax.rem(c + d // 4, 2), lax.rem(z + d % 4, 4))
            pltpu.make_async_remote_copy(
                src_ref=sca.at[ph, mya], dst_ref=sca.at[ph, mya], send_sem=s_sc_s.at[ph, 0],
                recv_sem=s_sc_r.at[ph, 0], device_id=to, device_id_type=MESH,
            ).start()

    def scalars_b(ph):
        wait_all(sca.at[ph, pl.ds(0, 7)], s_sc_r.at[ph, 0])
        total = sca[ph, 0]
        for i in range(1, 8):
            total += sca[ph, i]
        myb = x * 4 + yy
        scb[ph, myb] = total
        for d in range(1, 16):
            to = (lax.rem(x + d // 4, 4), lax.rem(yy + d % 4, 4), c, z)
            pltpu.make_async_remote_copy(
                src_ref=scb.at[ph, myb], dst_ref=scb.at[ph, myb], send_sem=s_sc_s.at[ph, 1],
                recv_sem=s_sc_r.at[ph, 1], device_id=to, device_id_type=MESH,
            ).start()

    def scalars_c(ph):
        wait_all(scb.at[ph, pl.ds(0, 15)], s_sc_r.at[ph, 1])
        total = scb[ph, 0]
        for i in range(1, 16):
            total += scb[ph, i]
        sums = jnp.sum(total, axis=1, keepdims=True)
        return sums[0:1], sums[1:2], sums[2:3]

    above, below = coords(s - 1), coords(s + 1)
    left, right = lax.rem(z + 3, 4), lax.rem(z + 1, 4)
    has_above, has_below = s > 0, s < 31

    def halo_copies(ph):
        def mk(n, src, dst, to):
            return pltpu.make_async_remote_copy(
                src_ref=src, dst_ref=dst, send_sem=s_halo_s.at[ph, n],
                recv_sem=s_halo_r.at[ph, n], device_id=to, device_id_type=MESH,
            )

        g = gp.at[ph]
        mid = pl.ds(8, LON)
        sides = [
            mk(0, est.at[ph, 0], hcol.at[ph, 1], (x, yy, c, left)),
            mk(1, est.at[ph, 1], hcol.at[ph, 0], (x, yy, c, right)),
        ]
        up = [
            mk(2, g.at[pl.ds(2, 2), mid], g.at[pl.ds(34, 2), mid], above + (z,)),
            mk(3, g.at[2, pl.ds(8, 8)], cn.at[ph, 0], above + (left,)),
            mk(4, g.at[2, pl.ds(64, 8)], cn.at[ph, 1], above + (right,)),
        ]
        down = [
            mk(5, g.at[pl.ds(32, 2), mid], g.at[pl.ds(0, 2), mid], below + (z,)),
            mk(6, g.at[33, pl.ds(8, 8)], cn.at[ph, 2], below + (left,)),
            mk(7, g.at[33, pl.ds(64, 8)], cn.at[ph, 3], below + (right,)),
        ]
        return sides, up, down

    def halo_send(ph):
        for r in range(LAT):
            g = jnp.where(sm_i[3, r] > 0, seg[sm_i[2, r]], 0.0)
            gp[ph, r + 2, 8:72, :] = g
            est[ph, 0, 2 * r : 2 * r + 2, :] = g[0:2]
            est[ph, 1, 2 * r : 2 * r + 2, :] = g[62:64]
        sides, up, down = halo_copies(ph)
        for cp in sides:
            cp.start()

        @pl.when(has_above)
        def _():
            for cp in up:
                cp.start()

        @pl.when(has_below)
        def _():
            for cp in down:
                cp.start()

    def halo_wait(ph):
        sides, up, down = halo_copies(ph)
        for cp in sides:
            cp.wait_recv()

        @pl.when(has_below)
        def _():
            for cp in up:
                cp.wait_recv()
            gp[ph, 34, 72:73, :] = cn[ph, 0, 0:1]
            gp[ph, 34, 7:8, :] = cn[ph, 1, 7:8]

        @pl.when(has_above)
        def _():
            for cp in down:
                cp.wait_recv()
            gp[ph, 1, 72:73, :] = cn[ph, 2, 0:1]
            gp[ph, 1, 7:8, :] = cn[ph, 3, 7:8]

        for r in range(LAT):
            gp[ph, r + 2, 72:74, :] = hcol[ph, 1, 2 * r : 2 * r + 2]
            gp[ph, r + 2, 6:8, :] = hcol[ph, 0, 2 * r : 2 * r + 2]

    def halo_done(ph):
        sides, up, down = halo_copies(ph)
        for cp in sides:
            cp.wait_send()

        @pl.when(has_above)
        def _():
            for cp in up:
                cp.wait_send()

        @pl.when(has_below)
        def _():
            for cp in down:
                cp.wait_send()

    sm = smooth[...]

    def smoothed(ref, r):
        v = ref[r]
        beside = ref[r - 1] + ref[r + 1] + pltpu.roll(v, 1, 0) + pltpu.roll(v, 79, 0)
        return v + sm * (beside - 4.0 * v)

    def inside(r):
        return ((r > 1) | has_above) & ((r < 34) | has_below)

    def squares(v):
        v = v * v
        t = v[0:8]
        for i in range(1, LON // 8):
            t += v[8 * i : 8 * i + 8]
        return t

    def to_forward(src):
        def step(r, total):
            u = smoothed(src, r)[8:72]
            hi, lo = split(u)
            u2[r - 2, 0:LON] = hi
            u2[r - 2, LON : 2 * LON] = lo
            return total + squares(src[r, 8:72, :])

        return sum8(lax.fori_loop(2, 34, step, jnp.zeros((8, 128), f32)))

    def slots_of(k):
        wait_spread(k)
        make_table(zt.at[k], tab)
        lookup(tab, oh, chan, pred, pc)
        image = hs[...] + pc[...]
        yw = w[...] * image
        y[...] = yw
        return sum8(yw * image)

    def term_y(b):
        return pred[:, lanes(b)] * y[pl.ds(b, 1), :]

    def term_d(b):
        p = pred[:, lanes(b)]
        return p * p * w[pl.ds(b, 1), :]

    bias_adjoint([term_y, term_d], chan, oh, lhs, acc)
    for t in range(TILES):
        rs0_send[t, 0:8] = acc_tile(acc, 0, t)
        rs0_send[t, 8:16] = acc_tile(acc, 1, t)
    pl.semaphore_wait(barrier, 127)
    scatter(rs0_send, rs0_recv, 0)
    to_smem.wait()
    load_j.wait()
    adjoint(y, jac, sm_i, cl, seg)
    halo_send(0)

    @pl.when(owner)
    def _():
        both = gathered(rs0_recv, 0)
        bp = biasp[:, lanes(lax.div(s, 3))]
        rb, dg = both[0:8], both[8:16] + bp
        zb = rb / dg
        ob[0] = rb
        ob[1] = dg
        ob[2] = zb
        ob[3] = bp
        zt[0, mine] = zb
        spread(0)

    halo_wait(0)

    def first(r, _):
        r0[r] = jnp.where(inside(r), smoothed(gp.at[0], r), 0.0)
        return 0

    lax.fori_loop(1, 35, first, 0)
    rr_state = to_forward(r0)

    forward(u2, jac, sm_i, cl, hs)
    d0 = slots_of(0)
    scalars_a(0, (
        rr_state + sum8(ob[0] * ob[2]),
        rr_state + d0 + sum8(ob[3] * ob[2] * ob[2]),
        rr_state + sum8(ob[0] * ob[0]),
    ))
    bias_adjoint([term_y], chan, oh, lhs, acc)
    for t in range(TILES):
        rs_send[0, t] = acc_tile(acc, 0, t)
    scatter(rs_send.at[0], rs_recv.at[0], 1)
    scalars_b(0)
    adjoint(y, jac, sm_i, cl, seg)
    halo_send(1)
    rz0, pq0, rr0 = scalars_c(0)
    alpha0 = rz0 / pq0

    @pl.when(owner)
    def _():
        qb = ob[3] * ob[2] + gathered(rs_recv.at[0], 1)
        rb = ob[0] - alpha0 * qb
        zb = rb / ob[1]
        ob[4] = qb
        ob[5] = rb
        ob[6] = zb
        zt[1, mine] = zb
        spread(1)

    halo_wait(1)

    def second(r, _):
        q = r0[r] + jnp.where(inside(r), smoothed(gp.at[1], r), 0.0)
        q0[r] = q
        r1[r] = r0[r] - alpha0 * q
        return 0

    lax.fori_loop(1, 35, second, 0)
    rr_state = to_forward(r1)

    forward(u2, jac, sm_i, cl, hs)
    d1 = slots_of(1)
    scalars_a(1, (
        rr_state + sum8(ob[5] * ob[6]),
        rr_state + d1 + sum8(ob[3] * ob[6] * ob[6]),
        rr_state + sum8(ob[5] * ob[5]),
    ))
    bias_adjoint([term_y], chan, oh, lhs, acc)
    for t in range(TILES):
        rs_send[1, t] = acc_tile(acc, 0, t)
    scatter(rs_send.at[1], rs_recv.at[1], 2)
    scalars_b(1)
    adjoint(y, jac, sm_i, cl, seg)
    halo_send(2)
    rz1, zaz, rr1 = scalars_c(1)
    beta = rz1 / rz0
    alpha1 = rz1 / (zaz - beta * rz1 / alpha0)
    mix = alpha0 + alpha1 * beta

    def solved(r, _):
        xs[r - 2] = mix * r0[r, 8:72, :] + alpha1 * r1[r, 8:72, :]
        return 0

    lax.fori_loop(2, 34, solved, 0)
    store_x = pltpu.make_async_copy(xs, out_x, s_load.at[2])
    store_x.start()
    for t in range(10):
        at = z * 10 + t
        out_b[:, t * 128 : (t + 1) * 128] = mix * zt[0, at] + alpha1 * zt[1, at]

    @pl.when(owner)
    def _():
        qb = ob[3] * ob[6] + gathered(rs_recv.at[1], 2) + beta * ob[4]
        ob[7] = ob[5] - alpha1 * qb

    halo_wait(2)

    def last(r, total):
        v = r1[r, 8:72, :]
        q = v + smoothed(gp.at[2], r)[8:72] + beta * q0[r, 8:72, :]
        return total + squares(v - alpha1 * q)

    rr_state = sum8(lax.fori_loop(2, 34, last, jnp.zeros((8, 128), f32)))
    scalars_a(2, (rr_state + sum8(ob[7] * ob[7]),))
    scalars_b(2)
    rr2, _, _ = scalars_c(2)
    lane = lax.broadcasted_iota(i32, (1, 128), 1)
    out_n[...] = jnp.sqrt(jnp.where(lane == 0, rr0, jnp.where(lane == 1, rr1, rr2)))

    for ph, ref in ((0, rs0_send), (1, rs_send.at[0]), (2, rs_send.at[1])):
        @pl.when(owner)
        def _(ph=ph, ref=ref):
            wait_all(ref.at[pl.ds(0, TILES - 1)], s_rs_s.at[ph])

        @pl.when(jnp.logical_not(owner))
        def _(ph=ph, ref=ref):
            wait_all(ref, s_rs_s.at[ph])

    @pl.when(owner)
    def _():
        for k in range(2):
            wait_all(rs_recv.at[0, pl.ds(0, 127)], s_ag_s.at[k])

    for ph in range(3):
        halo_done(ph)
        wait_all(sca.at[ph, pl.ds(0, 7)], s_sc_s.at[ph, 0])
        wait_all(scb.at[ph, pl.ds(0, 15)], s_sc_s.at[ph, 1])
    store_x.wait()


def body(innovations, obs_precision, jacobian, predictors, obs_column, obs_channel, obs_count, smoothing, bias_precision):
    vm = pl.BlockSpec(memory_space=pltpu.VMEM)
    hbm = pl.BlockSpec(memory_space=pl.ANY)
    sq = (LINES, 128)
    V = pltpu.VMEM
    D = pltpu.SemaphoreType.DMA
    out = pl.pallas_call(
        kernel,
        name="pcg",
        out_shape=(
            jax.ShapeDtypeStruct((LAT, LON, LEV), f32),
            jax.ShapeDtypeStruct((NPRED, 1280), f32),
            jax.ShapeDtypeStruct((1, 128), f32),
        ),
        in_specs=[vm, vm, hbm, vm, vm, vm, pl.BlockSpec(memory_space=pltpu.SMEM), vm, vm],
        out_specs=(hbm, vm, vm),
        scratch_shapes=[
            V((LINES, 128, LEV), bf16), V((LINES, 256, 128), bf16), V((KL, 640, 128), bf16), V((640, 256), f32), V((320, 256), bf16),
            V(sq, f32), V(sq, f32), V(sq, f32), V(sq, f32),
            V((LAT, 2 * LON, LEV), bf16), V((LINES, LON, LEV), f32),
            V((3, 36, 80, LEV), f32), V((36, 80, LEV), f32), V((36, 80, LEV), f32), V((36, 80, LEV), f32),
            V((LAT, LON, LEV), f32), V((3, 2, 64, LEV), f32), V((3, 2, 64, LEV), f32), V((3, 4, 8, LEV), f32),
            V((TILES, 16, 128), f32), V((128, 16, 128), f32), V((2, TILES, 8, 128), f32), V((2, 128, 8, 128), f32),
            V((2, TILES, 8, 128), f32), V((3, 8, 8, 128), f32), V((3, 16, 8, 128), f32), V((8, 8, 128), f32),
            V((8, 128), i32), V(sq, i32), pltpu.SMEM((8, 128), i32),
            D((3,)), D((3, 8)), D((3, 8)), D((3,)), D((3,)), D((2,)), D((2,)), D((3, 2)), D((3, 2)),
        ],
        compiler_params=pltpu.CompilerParams(
            collective_id=0, has_side_effects=True, vmem_limit_bytes=62 * 2**20
        ),
    )(
        innovations.reshape(sq), obs_precision.reshape(sq), jacobian.reshape(LINES, 128, LEV), predictors,
        obs_column.reshape(sq), obs_channel.reshape(sq), obs_count, smoothing.reshape(1, LEV), bias_precision,
    )
    return out[0], out[1], out[2][0, :3]


def solution(mesh):
    torus = Mesh(mesh.devices.reshape(4, 4, 2, mesh.shape["chan"]), AX)
    placed = (
        P(AX), P(AX), P(AX, None), P(None, AX), P(AX), P(AX), P(SWATH, "chan"), P(), P(None, "chan"),
    )
    return jax.shard_map(
        body,
        mesh=torus,
        in_specs=placed,
        out_specs=(P(SWATH, "chan", None), P(None, "chan"), P()),
        check_vma=False,
    )
```

```python
import jax
import jax.numpy as jnp
from jax import lax
from jax.experimental import pallas as pl
from jax.experimental.pallas import tpu as pltpu
from jax.sharding import Mesh
from jax.sharding import PartitionSpec as P

LEV = 128
NPRED = 8
LINES = 128
LAT = 32
LON = 64
TILES = 40
AX = ("swath_0", "swath_1", "swath_2", "chan")
SWATH = AX[:3]
MESH = pl.DeviceIdType.MESH
NT = (((1,), (1,)), ((), ()))
bf16, f32, i32 = jnp.bfloat16, jnp.float32, jnp.int32
KL = 32
UN = 32
PIECES = 4


def split(t):
    hi = t.astype(bf16)
    return hi, (t - hi.astype(f32)).astype(bf16)


def bc(row, n):
    return jnp.broadcast_to(row, (n, 128))


def lanes(b):
    return pl.ds(pl.multiple_of(b * 128, 128), 128)


def sum8(x):
    return jnp.sum(x, axis=0, keepdims=True)


def place(t):
    j = t % 10
    return (j % 2) * 20 + (t // 10) * 5 + j // 2


def make_table(zt, tab):
    for h in range(20):
        t = jnp.concatenate([zt[place(2 * h)], zt[place(2 * h + 1)]], axis=1)
        tab[16 * h : 16 * h + 16] = jnp.concatenate(split(t), axis=0)


def lookup(tab, oh, ch_ref, pred_ref, out_ref):
    def step(i, _):
        for g in range(UN // 2):
            b0 = i * UN + 2 * g
            hot = jnp.concatenate([oh[b0], oh[b0 + 1]], axis=1)
            got = jnp.dot(tab[...], hot, preferred_element_type=f32)
            for u in range(2):
                b, ls = b0 + u, slice(u * 128, u * 128 + 128)
                hb = bc(ch_ref[pl.ds(b, 1), :] >> 8, 8)
                hi = jnp.zeros((8, 128), f32)
                lo = hi
                for h in range(20):
                    m = hb == h
                    hi = jnp.where(m, got[16 * h : 16 * h + 8, ls], hi)
                    lo = jnp.where(m, got[16 * h + 8 : 16 * h + 16, ls], lo)
                out_ref[pl.ds(b, 1), :] = sum8((hi + lo) * pred_ref[:, lanes(b)])
        return 0

    lax.fori_loop(0, LINES // UN, step, 0)


def forward(u2, jac, sm_i, col_ref, out_ref):
    iota = lax.broadcasted_iota(i32, (LON, 128), 0)

    def step(i, _):
        for g in range(UN // 2):
            b0 = i * UN + 2 * g
            left = jnp.concatenate([u2[sm_i[4, b0]], u2[sm_i[4, b0 + 1]]], axis=0)
            pair = jnp.concatenate([jac[b0], jac[b0 + 1]], axis=0)
            both = lax.dot_general(left, pair, NT, preferred_element_type=f32)
            for u in range(2):
                b, at = b0 + u, 128 * u
                mine = both[at : at + 128, at : at + 128]
                m = iota == bc(col_ref[pl.ds(b, 1), :], LON)
                out_ref[pl.ds(b, 1), :] = sum8(jnp.where(m, mine[:LON] + mine[LON:], 0.0))
        return 0

    lax.fori_loop(0, LINES // UN, step, 0)


def adjoint(y_ref, jac, sm_i, col_ref, seg):
    iota = lax.broadcasted_iota(i32, (LON, 128), 0)

    def step(i, acc):
        for u in range(UN):
            k = i * UN + u
            b = sm_i[0, k]
            y = y_ref[pl.ds(b, 1), :]
            hi = y.astype(bf16).astype(f32)
            lo = y - hi
            m = iota == bc(col_ref[pl.ds(b, 1), :], LON)
            parts = [jnp.where(m, bc(t, LON), 0.0) for t in (hi, lo)]
            a = jnp.concatenate(parts, axis=0).astype(bf16)
            both = jnp.dot(a, jac[b], preferred_element_type=f32)
            same = sm_i[1, k] == sm_i[1, jnp.maximum(k - 1, 0)]
            acc = jnp.where(same, acc, 0.0) + (both[:LON] + both[LON:])
            seg[k] = acc
        return acc

    lax.fori_loop(0, LINES // UN, step, jnp.zeros((LON, 128), f32))


def make_hot(ch_ref, oh):
    iota = lax.broadcasted_iota(i32, (256, 128), 0).astype(f32).astype(bf16)
    one, zero = jnp.ones((), bf16), jnp.zeros((), bf16)

    def step(i, _):
        for u in range(8):
            b = i * 8 + u
            ch = bc((ch_ref[pl.ds(b, 1), :] & 255).astype(f32), 16).astype(bf16)
            for j in range(0, 256, 16):
                oh[b, j : j + 16] = jnp.where(iota[j : j + 16] == ch, one, zero)
        return 0

    lax.fori_loop(0, LINES // 8, step, 0)


def bias_adjoint(terms, ch_ref, oh, lhs, acc):
    n = len(terms)
    rows, kl = 320 * n, KL // n
    zero = jnp.zeros((), bf16)

    def step(c, _):
        for l in range(kl):
            b = c * kl + l
            hb = bc((ch_ref[pl.ds(b, 1), :] >> 8).astype(f32), 16).astype(bf16)
            sts = [jnp.concatenate(split(f(b)), axis=0) for f in terms]
            for h in range(20):
                m = hb == jnp.asarray(h, bf16)
                for j, st in enumerate(sts):
                    at = (j * 20 + h) * 16
                    lhs[l, at : at + 16] = jnp.where(m, st, zero)
        left = jnp.concatenate([lhs[l, :rows] for l in range(kl)], axis=1)
        hot = jnp.concatenate([oh[c * kl + l] for l in range(kl)], axis=1)
        acc[:rows] += lax.dot_general(left, hot, NT, preferred_element_type=f32)
        return 0

    acc[:rows] = jnp.zeros((rows, 256), f32)
    lax.fori_loop(0, LINES // kl, step, 0)


def acc_tile(acc, j, t):
    at, ls = (j * 20 + t // 2) * 16, slice((t % 2) * 128, (t % 2) * 128 + 128)
    return acc[at : at + 8, ls] + acc[at + 8 : at + 16, ls]


def wait_all(ref, sem):
    pltpu.make_async_copy(ref, ref, sem).wait()


def kernel(
    innov_hbm, prec_hbm, jac_hbm, pred_hbm, col_hbm, chan_hbm, count, smooth_hbm, biasp_hbm,
    out_x, out_b, out_n,
    innov, prec, pred, col, chan, smooth, biasp, jac, oh, lhs, acc, tab, w, y, hs, pc, u2, seg, gp, r0, r1, q0, xs, est, hcol, cn,
    rs0_send, pr0, rs0_recv, rs_send, pr, rs_recv, zt, sp, sc, ob, iv, cl, sm_i,
    s_load, s_halo_s, s_halo_r, s_pr_s, s_pr_r, s_rs_s, s_rs_r, s_ag_s, s_ag_r, s_rl_s, s_rl_r,
    s_sp_s, s_sp_r, s_sc_s, s_sc_r,
):
    x, yy, c, z = (lax.axis_index(a) for a in AX)
    s = (x * 4 + yy) * 2 + c
    owner = (lax.rem(s, 3) == 0) & (s < 30)
    half = c * 20
    mine = half + z * 5 + lax.div(s, 6)
    chip = (x * 4 + yy) * 4 + z
    partner = (x, yy, 1 - c, z)
    xs4 = [lax.rem(x + d, 4) for d in range(4)]
    ys4 = [lax.rem(yy + d, 4) for d in range(4)]
    zs4 = [lax.rem(z + d, 4) for d in range(4)]

    def coords(sw):
        return lax.div(sw, 8), lax.rem(lax.div(sw, 2), 4), lax.rem(sw, 2)

    pairs = (
        (innov_hbm, innov), (prec_hbm, prec), (col_hbm, col), (chan_hbm, chan), (pred_hbm, pred),
        (smooth_hbm, smooth), (biasp_hbm, biasp), (jac_hbm, jac),
    )
    loads = [pltpu.make_async_copy(a, b, s_load.at[i]) for i, (a, b) in enumerate(pairs)]
    for cp in loads:
        cp.start()
    for ph in range(3):
        for r in (0, 1, 34, 35):
            gp[ph, r] = jnp.zeros((80, 128), f32)

    def chips(f):
        for d in range(1, 64):
            f((xs4[d // 16], ys4[d // 4 % 4], c, zs4[d % 4]))

    above, below = coords(s - 1), coords(s + 1)
    left, right = zs4[3], zs4[1]
    has_above, has_below = s > 0, s < 31

    barrier = pltpu.get_barrier_semaphore()

    def greet(to):
        pl.semaphore_signal(barrier, inc=1, device_id=to, device_id_type=MESH)

    chips(greet)
    for there, side in ((has_above, above), (has_below, below)):
        @pl.when(there)
        def _(side=side):
            for to_z in (z, left, right):
                greet(side + (to_z,))

    greeted = 63 + jnp.where(has_above, 3, 0) + jnp.where(has_below, 3, 0)

    for cp in loads[:7]:
        cp.wait()
    slot = lax.broadcasted_iota(i32, (LINES, 128), 0) * 128 + lax.broadcasted_iota(i32, (LINES, 128), 1)
    w[...] = jnp.where(slot < count[0, 0], prec[...], 0.0)
    y[...] = w[...] * innov[...]

    iota_s = lax.broadcasted_iota(i32, (128, 128), 0)
    iota_l = lax.broadcasted_iota(i32, (128, 128), 1)

    def count_of(m, v=1):
        return sum8(jnp.where(m, v, 0))

    a = jnp.broadcast_to(col[:, 0:1] >> 6, (128, 128))
    row_l = count_of(iota_s == iota_l, a)
    b = bc(row_l, 128)
    rank = jnp.transpose(bc(count_of((a < b) | ((a == b) & (iota_s < iota_l))), 128))
    put = rank == iota_l
    iv[0:1] = count_of(put, iota_s)
    iv[1:2] = count_of(put, a)
    iv[2:3] = jnp.maximum(count_of(a <= iota_l) - 1, 0)
    iv[3:4] = count_of(a == iota_l)
    iv[4:5] = row_l
    iv[5:8] = jnp.zeros((3, 128), i32)
    to_smem = pltpu.make_async_copy(iv, sm_i, s_load.at[8])
    to_smem.start()
    make_hot(chan, oh)
    cl[...] = col[...] & 63

    for i in range(8):
        ob[i] = jnp.zeros((8, 128), f32)

    def pair_send(send, pair, ph):
        pltpu.make_async_remote_copy(
            src_ref=send.at[pl.ds(20 - half, 20)], dst_ref=pair, send_sem=s_pr_s.at[ph],
            recv_sem=s_pr_r.at[ph], device_id=partner, device_id_type=MESH,
        ).start()

    def scatter(send, pair, recv, ph):
        wait_all(pair, s_pr_r.at[ph])
        for i in range(20):
            pair[i] = pair[i] + send[half + i]
        for i in range(20):
            tz = zs4[i // 5]
            jj = lax.rem(x + yy + i % 5, 5)
            sw = 6 * jj + 3 * c
            tx, ty = lax.div(sw, 8), lax.rem(lax.div(sw, 2), 4)
            away = (tx != x) | (ty != yy) | (tz != z)

            @pl.when(away)
            def _(tz=tz, jj=jj, tx=tx, ty=ty):
                pltpu.make_async_remote_copy(
                    src_ref=pair.at[tz * 5 + jj], dst_ref=recv.at[chip], send_sem=s_rs_s.at[ph],
                    recv_sem=s_rs_r.at[ph], device_id=(tx, ty, c, tz), device_id_type=MESH,
                ).start()

        @pl.when(owner)
        def _():
            recv[chip] = pair[mine - half]

    def gathered(recv, ph):
        wait_all(recv.at[pl.ds(0, 63)], s_rs_r.at[ph])
        parts = [recv[i] for i in range(4)]
        for i in range(4, 64):
            parts[i % 4] += recv[i]
        return (parts[0] + parts[1]) + (parts[2] + parts[3])

    def spread(k):
        def send(to):
            pltpu.make_async_remote_copy(
                src_ref=zt.at[k, mine], dst_ref=zt.at[k, mine], send_sem=s_ag_s.at[k],
                recv_sem=s_ag_r.at[k], device_id=to, device_id_type=MESH,
            ).start()

        chips(send)

    def relay(k):
        ours = zt.at[k, pl.ds(half, 20)]
        return pltpu.make_async_remote_copy(
            src_ref=ours, dst_ref=ours, send_sem=s_rl_s.at[k], recv_sem=s_rl_r.at[k],
            device_id=partner, device_id_type=MESH,
        )

    def wait_spread(k):
        @pl.when(owner)
        def _():
            wait_all(zt.at[k, pl.ds(0, 19)], s_ag_r.at[k])

        @pl.when(jnp.logical_not(owner))
        def _():
            wait_all(zt.at[k, pl.ds(0, 20)], s_ag_r.at[k])

        relay(k).start()
        wait_all(zt.at[k, pl.ds(0, 20)], s_rl_r.at[k])

    lane = lax.broadcasted_iota(i32, (1, 128), 1)

    def scalar_pair(ph):
        return pltpu.make_async_remote_copy(
            src_ref=sp.at[ph, 0], dst_ref=sp.at[ph, 1], send_sem=s_sp_s.at[ph],
            recv_sem=s_sp_r.at[ph], device_id=partner, device_id_type=MESH,
        )

    def scalars_a(ph, rows):
        row = jnp.zeros((1, 128), f32)
        for i, r in enumerate(rows):
            row = jnp.where(lane == i, jnp.sum(r, axis=1, keepdims=True), row)
        sp[ph, 0] = row
        scalar_pair(ph).start()

    def scalars_b(ph):
        scalar_pair(ph).wait_recv()
        sc[ph, chip] = sp[ph, 0] + sp[ph, 1]

        def send(to):
            pltpu.make_async_remote_copy(
                src_ref=sc.at[ph, chip], dst_ref=sc.at[ph, chip], send_sem=s_sc_s.at[ph],
                recv_sem=s_sc_r.at[ph], device_id=to, device_id_type=MESH,
            ).start()

        chips(send)

    def scalars_c(ph):
        wait_all(sc.at[ph, pl.ds(0, 63)], s_sc_r.at[ph])
        parts = [sc[ph, i] for i in range(4)]
        for i in range(4, 64):
            parts[i % 4] += sc[ph, i]
        total = (parts[0] + parts[1]) + (parts[2] + parts[3])
        return tuple(jnp.broadcast_to(total[:, i : i + 1], (1, 128)) for i in range(3))

    def halo_copies(ph):
        def mk(n, src, dst, to):
            return pltpu.make_async_remote_copy(
                src_ref=src, dst_ref=dst, send_sem=s_halo_s.at[ph, n],
                recv_sem=s_halo_r.at[ph, n], device_id=to, device_id_type=MESH,
            )

        g = gp.at[ph]
        mid = pl.ds(8, LON)
        sides = [
            mk(0, est.at[ph, 0], hcol.at[ph, 1], (x, yy, c, left)),
            mk(1, est.at[ph, 1], hcol.at[ph, 0], (x, yy, c, right)),
        ]
        up = [
            mk(2, g.at[pl.ds(2, 2), mid], g.at[pl.ds(34, 2), mid], above + (z,)),
            mk(3, g.at[2, pl.ds(8, 8)], cn.at[ph, 0], above + (left,)),
            mk(4, g.at[2, pl.ds(64, 8)], cn.at[ph, 1], above + (right,)),
        ]
        down = [
            mk(5, g.at[pl.ds(32, 2), mid], g.at[pl.ds(0, 2), mid], below + (z,)),
            mk(6, g.at[33, pl.ds(8, 8)], cn.at[ph, 2], below + (left,)),
            mk(7, g.at[33, pl.ds(64, 8)], cn.at[ph, 3], below + (right,)),
        ]
        return sides, up, down

    def halo_send(ph):
        for r in range(LAT):
            g = jnp.where(sm_i[3, r] > 0, seg[sm_i[2, r]], 0.0)
            gp[ph, r + 2, 8:72, :] = g
            est[ph, 0, 2 * r : 2 * r + 2, :] = g[0:2]
            est[ph, 1, 2 * r : 2 * r + 2, :] = g[62:64]
        sides, up, down = halo_copies(ph)
        for cp in sides:
            cp.start()

        @pl.when(has_above)
        def _():
            for cp in up:
                cp.start()

        @pl.when(has_below)
        def _():
            for cp in down:
                cp.start()

    def halo_wait(ph):
        sides, up, down = halo_copies(ph)
        for cp in sides:
            cp.wait_recv()

        @pl.when(has_below)
        def _():
            for cp in up:
                cp.wait_recv()
            gp[ph, 34, 72:73, :] = cn[ph, 0, 0:1]
            gp[ph, 34, 7:8, :] = cn[ph, 1, 7:8]

        @pl.when(has_above)
        def _():
            for cp in down:
                cp.wait_recv()
            gp[ph, 1, 72:73, :] = cn[ph, 2, 0:1]
            gp[ph, 1, 7:8, :] = cn[ph, 3, 7:8]

        for r in range(LAT):
            gp[ph, r + 2, 72:74, :] = hcol[ph, 1, 2 * r : 2 * r + 2]
            gp[ph, r + 2, 6:8, :] = hcol[ph, 0, 2 * r : 2 * r + 2]

    def halo_done(ph):
        sides, up, down = halo_copies(ph)
        for cp in sides:
            cp.wait_send()

        @pl.when(has_above)
        def _():
            for cp in up:
                cp.wait_send()

        @pl.when(has_below)
        def _():
            for cp in down:
                cp.wait_send()

    sm = smooth[...]

    def smoothed(ref, r):
        v = ref[r]
        beside = ref[r - 1] + ref[r + 1] + pltpu.roll(v, 1, 0) + pltpu.roll(v, 79, 0)
        return v + sm * (beside - 4.0 * v)

    def inside(r):
        return ((r > 1) | has_above) & ((r < 34) | has_below)

    def squares(v):
        v = v * v
        t = v[0:8]
        for i in range(1, LON // 8):
            t += v[8 * i : 8 * i + 8]
        return t

    def to_forward(src):
        def step(r, total):
            u = smoothed(src, r)[8:72]
            hi, lo = split(u)
            u2[r - 2, 0:LON] = hi
            u2[r - 2, LON : 2 * LON] = lo
            return total + squares(src[r, 8:72, :])

        return sum8(lax.fori_loop(2, 34, step, jnp.zeros((8, 128), f32)))

    def slots_of(k):
        wait_spread(k)
        make_table(zt.at[k], tab)
        lookup(tab, oh, chan, pred, pc)
        image = hs[...] + pc[...]
        yw = w[...] * image
        y[...] = yw
        return sum8(yw * image)

    def term_y(b):
        return pred[:, lanes(b)] * y[pl.ds(b, 1), :]

    def term_d(b):
        p = pred[:, lanes(b)]
        return p * p * w[pl.ds(b, 1), :]

    bias_adjoint([term_y, term_d], chan, oh, lhs, acc)
    for t in range(TILES):
        rs0_send[place(t), 0:8] = acc_tile(acc, 0, t)
        rs0_send[place(t), 8:16] = acc_tile(acc, 1, t)
    pl.semaphore_wait(barrier, greeted)
    pair_send(rs0_send, pr0, 0)
    to_smem.wait()
    loads[7].wait()
    scatter(rs0_send, pr0, rs0_recv, 0)
    adjoint(y, jac, sm_i, cl, seg)
    halo_send(0)

    @pl.when(owner)
    def _():
        both = gathered(rs0_recv, 0)
        bp = biasp[:, lanes(lax.div(s, 3))]
        rb, dg = both[0:8], both[8:16] + bp
        zb = rb / dg
        ob[0] = rb
        ob[1] = dg
        ob[2] = zb
        ob[3] = bp
        zt[0, mine] = zb
        spread(0)

    halo_wait(0)

    def first(r, _):
        r0[r] = jnp.where(inside(r), smoothed(gp.at[0], r), 0.0)
        return 0

    lax.fori_loop(1, 35, first, 0)
    rr_state = to_forward(r0)

    forward(u2, jac, sm_i, cl, hs)
    d0 = slots_of(0)
    scalars_a(0, (
        rr_state + sum8(ob[0] * ob[2]),
        rr_state + d0 + sum8(ob[3] * ob[2] * ob[2]),
        rr_state + sum8(ob[0] * ob[0]),
    ))
    bias_adjoint([term_y], chan, oh, lhs, acc)
    for t in range(TILES):
        rs_send[0, place(t)] = acc_tile(acc, 0, t)
    pair_send(rs_send.at[0], pr.at[0], 1)
    scatter(rs_send.at[0], pr.at[0], rs_recv.at[0], 1)
    scalars_b(0)
    adjoint(y, jac, sm_i, cl, seg)
    halo_send(1)
    rz0, pq0, rr0 = scalars_c(0)
    alpha0 = rz0 / pq0

    @pl.when(owner)
    def _():
        qb = ob[3] * ob[2] + gathered(rs_recv.at[0], 1)
        rb = ob[0] - alpha0 * qb
        zb = rb / ob[1]
        ob[4] = qb
        ob[5] = rb
        ob[6] = zb
        zt[1, mine] = zb
        spread(1)

    halo_wait(1)

    def second(r, _):
        q = r0[r] + jnp.where(inside(r), smoothed(gp.at[1], r), 0.0)
        q0[r] = q
        r1[r] = r0[r] - alpha0 * q
        return 0

    lax.fori_loop(1, 35, second, 0)
    rr_state = to_forward(r1)

    forward(u2, jac, sm_i, cl, hs)
    d1 = slots_of(1)
    scalars_a(1, (
        rr_state + sum8(ob[5] * ob[6]),
        rr_state + d1 + sum8(ob[3] * ob[6] * ob[6]),
        rr_state + sum8(ob[5] * ob[5]),
    ))
    bias_adjoint([term_y], chan, oh, lhs, acc)
    for t in range(TILES):
        rs_send[1, place(t)] = acc_tile(acc, 0, t)
    pair_send(rs_send.at[1], pr.at[1], 2)
    scatter(rs_send.at[1], pr.at[1], rs_recv.at[1], 2)
    scalars_b(1)
    adjoint(y, jac, sm_i, cl, seg)
    halo_send(2)
    rz1, zaz, rr1 = scalars_c(1)
    beta = rz1 / rz0
    alpha1 = rz1 / (zaz - beta * rz1 / alpha0)
    mix = alpha0 + alpha1 * beta

    def solved(r, _):
        xs[r - 2] = mix * r0[r, 8:72, :] + alpha1 * r1[r, 8:72, :]
        return 0

    lax.fori_loop(2, 34, solved, 0)
    store_x = pltpu.make_async_copy(xs, out_x, s_load.at[9])
    store_x.start()
    for t in range(10):
        at = (t % 2) * 20 + z * 5 + t // 2
        out_b[:, t * 128 : (t + 1) * 128] = mix * zt[0, at] + alpha1 * zt[1, at]

    @pl.when(owner)
    def _():
        qb = ob[3] * ob[6] + gathered(rs_recv.at[1], 2) + beta * ob[4]
        ob[7] = ob[5] - alpha1 * qb

    halo_wait(2)

    def last(r, total):
        v = r1[r, 8:72, :]
        q = v + smoothed(gp.at[2], r)[8:72] + beta * q0[r, 8:72, :]
        return total + squares(v - alpha1 * q)

    rr_state = sum8(lax.fori_loop(2, 34, last, jnp.zeros((8, 128), f32)))
    scalars_a(2, (rr_state + sum8(ob[7] * ob[7]),))
    scalars_b(2)
    rr2, _, _ = scalars_c(2)
    out_n[...] = jnp.sqrt(jnp.where(lane == 0, rr0, jnp.where(lane == 1, rr1, rr2)))

    for ph, ref in ((0, pr0), (1, pr.at[0]), (2, pr.at[1])):
        wait_all(ref, s_pr_s.at[ph])

        @pl.when(owner)
        def _(ph=ph, ref=ref):
            wait_all(ref.at[pl.ds(0, 19)], s_rs_s.at[ph])

        @pl.when(jnp.logical_not(owner))
        def _(ph=ph, ref=ref):
            wait_all(ref, s_rs_s.at[ph])

    @pl.when(owner)
    def _():
        for k in range(2):
            wait_all(rs_recv.at[0, pl.ds(0, 63)], s_ag_s.at[k])

    for k in range(2):
        relay(k).wait_send()
    for ph in range(3):
        halo_done(ph)
        scalar_pair(ph).wait_send()
        wait_all(sc.at[ph, pl.ds(0, 63)], s_sc_s.at[ph])
    store_x.wait()


def finish(x_in, b_in, n_in, x_out, b_out, n_out, hold, held_b, sem):
    first = pltpu.make_async_copy(b_in, held_b, sem.at[0])
    first.start()
    rows = LAT // PIECES
    come = []
    for i in range(PIECES):
        part = pl.ds(i * rows, rows)
        cp = pltpu.make_async_copy(x_in.at[part], hold.at[part], sem.at[2 + i])
        cp.start()
        come.append(cp)
    n_out[...] = n_in[:, 0:3]
    first.wait()
    second = pltpu.make_async_copy(held_b, b_out, sem.at[1])
    second.start()
    go = [second]
    for i, cp in enumerate(come):
        part = pl.ds(i * rows, rows)
        cp.wait()
        out = pltpu.make_async_copy(hold.at[part], x_out.at[part], sem.at[2 + PIECES + i])
        out.start()
        go.append(out)
    for cp in go:
        cp.wait()


def body(innovations, obs_precision, jacobian, predictors, obs_column, obs_channel, obs_count, smoothing, bias_precision):
    vm = pl.BlockSpec(memory_space=pltpu.VMEM)
    hbm = pl.BlockSpec(memory_space=pl.ANY)
    src = pl.BlockSpec(memory_space=pltpu.HBM)
    sq = (LINES, 128)
    V = pltpu.VMEM
    D = pltpu.SemaphoreType.DMA
    out = pl.pallas_call(
        kernel,
        name="pcg",
        out_shape=(
            jax.ShapeDtypeStruct((LAT, LON, LEV), f32),
            jax.ShapeDtypeStruct((NPRED, 1280), f32),
            jax.ShapeDtypeStruct((1, 128), f32),
        ),
        in_specs=[src] * 6 + [pl.BlockSpec(memory_space=pltpu.SMEM), src, src],
        out_specs=(hbm, vm, vm),
        scratch_shapes=[
            V(sq, f32), V(sq, f32), V((NPRED, 16384), f32), V(sq, i32), V(sq, i32), V((1, LEV), f32), V((NPRED, 1280), f32),
            V((LINES, 128, LEV), bf16), V((LINES, 256, 128), bf16), V((KL, 640, 128), bf16), V((640, 256), f32), V((320, 256), bf16),
            V(sq, f32), V(sq, f32), V(sq, f32), V(sq, f32),
            V((LAT, 2 * LON, LEV), bf16), V((LINES, LON, LEV), f32),
            V((3, 36, 80, LEV), f32), V((36, 80, LEV), f32), V((36, 80, LEV), f32), V((36, 80, LEV), f32),
            V((LAT, LON, LEV), f32), V((3, 2, 64, LEV), f32), V((3, 2, 64, LEV), f32), V((3, 4, 8, LEV), f32),
            V((TILES, 16, 128), f32), V((20, 16, 128), f32), V((64, 16, 128), f32),
            V((2, TILES, 8, 128), f32), V((2, 20, 8, 128), f32), V((2, 64, 8, 128), f32),
            V((2, TILES, 8, 128), f32), V((3, 2, 1, 128), f32), V((3, 64, 1, 128), f32), V((8, 8, 128), f32),
            V((8, 128), i32), V(sq, i32), pltpu.SMEM((8, 128), i32),
            D((10,)), D((3, 8)), D((3, 8)), D((3,)), D((3,)), D((3,)), D((3,)), D((2,)), D((2,)), D((2,)), D((2,)),
            D((3,)), D((3,)), D((3,)), D((3,)),
        ],
        compiler_params=pltpu.CompilerParams(
            collective_id=0, has_side_effects=True, vmem_limit_bytes=62 * 2**20
        ),
    )(
        innovations.reshape(sq), obs_precision.reshape(sq), jacobian.reshape(LINES, 128, LEV), predictors,
        obs_column.reshape(sq), obs_channel.reshape(sq), obs_count, smoothing.reshape(1, LEV), bias_precision,
    )
    done = pl.pallas_call(
        finish,
        name="finish",
        out_shape=(
            jax.ShapeDtypeStruct((LAT, LON, LEV), f32),
            jax.ShapeDtypeStruct((NPRED, 1280), f32),
            jax.ShapeDtypeStruct((1, 3), f32),
        ),
        in_specs=[hbm, hbm, vm],
        out_specs=(hbm, hbm, vm),
        scratch_shapes=[V((LAT, LON, LEV), f32), V((NPRED, 1280), f32), D((2 + 2 * PIECES,))],
        compiler_params=pltpu.CompilerParams(vmem_limit_bytes=62 * 2**20),
    )(*out)
    return done[0], done[1], done[2][0]


def solution(mesh):
    torus = Mesh(mesh.devices.reshape(4, 4, 2, mesh.shape["chan"]), AX)
    placed = (
        P(AX), P(AX), P(AX, None), P(None, AX), P(AX), P(AX), P(SWATH, "chan"), P(), P(None, "chan"),
    )
    return jax.shard_map(
        body,
        mesh=torus,
        in_specs=placed,
        out_specs=(P(SWATH, "chan", None), P(None, "chan"), P()),
        check_vma=False,
    )
```

```python
import jax
import jax.numpy as jnp
from jax import lax
from jax.experimental import pallas as pl
from jax.experimental.pallas import tpu as pltpu
from jax.sharding import Mesh
from jax.sharding import PartitionSpec as P

LEV = 128
NPRED = 8
LINES = 128
LAT = 32
LON = 64
TILES = 40
AX = ("swath_0", "swath_1", "swath_2", "chan")
SWATH = AX[:3]
MESH = pl.DeviceIdType.MESH
NT = (((1,), (1,)), ((), ()))
bf16, f32, i32 = jnp.bfloat16, jnp.float32, jnp.int32
KL = 32
UN = 32
PIECES = 4


def split(t):
    hi = t.astype(bf16)
    return hi, (t - hi.astype(f32)).astype(bf16)


def bc(row, n):
    return jnp.broadcast_to(row, (n, 128))


def lanes(b):
    return pl.ds(pl.multiple_of(b * 128, 128), 128)


def sum8(x):
    return jnp.sum(x, axis=0, keepdims=True)


def place(t):
    j = t % 10
    return (j % 2) * 20 + (t // 10) * 5 + j // 2


def make_table(zt, tab):
    for h in range(20):
        t = jnp.concatenate([zt[place(2 * h)], zt[place(2 * h + 1)]], axis=1)
        tab[16 * h : 16 * h + 16] = jnp.concatenate(split(t), axis=0)


def lookup(tab, oh, ch_ref, pred_ref, out_ref):
    def step(i, _):
        for g in range(UN // 2):
            b0 = i * UN + 2 * g
            hot = jnp.concatenate([oh[b0], oh[b0 + 1]], axis=1)
            got = jnp.dot(tab[...], hot, preferred_element_type=f32)
            for u in range(2):
                b, ls = b0 + u, slice(u * 128, u * 128 + 128)
                hb = bc(ch_ref[pl.ds(b, 1), :] >> 8, 8)
                hi = jnp.zeros((8, 128), f32)
                lo = hi
                for h in range(20):
                    m = hb == h
                    hi = jnp.where(m, got[16 * h : 16 * h + 8, ls], hi)
                    lo = jnp.where(m, got[16 * h + 8 : 16 * h + 16, ls], lo)
                out_ref[pl.ds(b, 1), :] = sum8((hi + lo) * pred_ref[:, lanes(b)])
        return 0

    lax.fori_loop(0, LINES // UN, step, 0)


def forward(u2, jac, sm_i, col_ref, out_ref):
    iota = lax.broadcasted_iota(i32, (LON, 128), 0)

    def step(i, _):
        for g in range(UN // 2):
            b0 = i * UN + 2 * g
            left = jnp.concatenate([u2[sm_i[4, b0]], u2[sm_i[4, b0 + 1]]], axis=0)
            pair = jnp.concatenate([jac[b0], jac[b0 + 1]], axis=0)
            both = lax.dot_general(left, pair, NT, preferred_element_type=f32)
            for u in range(2):
                b, at = b0 + u, 128 * u
                mine = both[at : at + 128, at : at + 128]
                m = iota == bc(col_ref[pl.ds(b, 1), :], LON)
                out_ref[pl.ds(b, 1), :] = sum8(jnp.where(m, mine[:LON] + mine[LON:], 0.0))
        return 0

    lax.fori_loop(0, LINES // UN, step, 0)


def adjoint(y_ref, jac, sm_i, col_ref, seg):
    iota = lax.broadcasted_iota(i32, (LON, 128), 0)

    def step(i, acc):
        for u in range(UN):
            k = i * UN + u
            b = sm_i[0, k]
            y = y_ref[pl.ds(b, 1), :]
            hi = y.astype(bf16).astype(f32)
            lo = y - hi
            m = iota == bc(col_ref[pl.ds(b, 1), :], LON)
            parts = [jnp.where(m, bc(t, LON), 0.0) for t in (hi, lo)]
            a = jnp.concatenate(parts, axis=0).astype(bf16)
            both = jnp.dot(a, jac[b], preferred_element_type=f32)
            same = sm_i[1, k] == sm_i[1, jnp.maximum(k - 1, 0)]
            acc = jnp.where(same, acc, 0.0) + (both[:LON] + both[LON:])
            seg[k] = acc
        return acc

    lax.fori_loop(0, LINES // UN, step, jnp.zeros((LON, 128), f32))


def bias_adjoint(terms, ch_ref, oh, lhs, acc, fill=False):
    n = len(terms)
    rows, kl = 320 * n, KL // n
    one, zero = jnp.ones((), bf16), jnp.zeros((), bf16)
    iota = lax.broadcasted_iota(i32, (256, 128), 0).astype(f32).astype(bf16)

    def step(c, _):
        for l in range(kl):
            b = c * kl + l
            hb = bc((ch_ref[pl.ds(b, 1), :] >> 8).astype(f32), 16).astype(bf16)
            if fill:
                ch = bc((ch_ref[pl.ds(b, 1), :] & 255).astype(f32), 16).astype(bf16)
                for j in range(0, 256, 16):
                    oh[b, j : j + 16] = jnp.where(iota[j : j + 16] == ch, one, zero)
            sts = [jnp.concatenate(split(f(b)), axis=0) for f in terms]
            for h in range(20):
                m = hb == jnp.asarray(h, bf16)
                for j, st in enumerate(sts):
                    at = (j * 20 + h) * 16
                    lhs[l, at : at + 16] = jnp.where(m, st, zero)
        left = jnp.concatenate([lhs[l, :rows] for l in range(kl)], axis=1)
        hot = jnp.concatenate([oh[c * kl + l] for l in range(kl)], axis=1)
        acc[:rows] += lax.dot_general(left, hot, NT, preferred_element_type=f32)
        return 0

    acc[:rows] = jnp.zeros((rows, 256), f32)
    lax.fori_loop(0, LINES // kl, step, 0)


def acc_tile(acc, j, t):
    at, ls = (j * 20 + t // 2) * 16, slice((t % 2) * 128, (t % 2) * 128 + 128)
    return acc[at : at + 8, ls] + acc[at + 8 : at + 16, ls]


def wait_all(ref, sem):
    pltpu.make_async_copy(ref, ref, sem).wait()


def kernel(
    innov_hbm, prec_hbm, jac_hbm, pred_hbm, col_hbm, chan_hbm, count, smooth_hbm, biasp_hbm,
    out_x, out_b, out_n,
    innov, prec, pred, col, chan, smooth, biasp, jac, oh, lhs, acc, tab, w, y, hs, pc, u2, seg, gp, r0, r1, q0, xs, est, hcol, cn,
    rs0_send, pr0, rs0_recv, rs_send, pr, rs_recv, zt, sp, sc, ob, iv, cl, sm_i,
    s_load, s_halo_s, s_halo_r, s_pr_s, s_pr_r, s_rs_s, s_rs_r, s_ag_s, s_ag_r, s_rl_s, s_rl_r,
    s_sp_s, s_sp_r, s_sc_s, s_sc_r,
):
    x, yy, c, z = (lax.axis_index(a) for a in AX)
    s = (x * 4 + yy) * 2 + c
    owner = (lax.rem(s, 3) == 0) & (s < 30)
    half = c * 20
    mine = half + z * 5 + lax.div(s, 6)
    chip = (x * 4 + yy) * 4 + z
    partner = (x, yy, 1 - c, z)
    xs4 = [lax.rem(x + d, 4) for d in range(4)]
    ys4 = [lax.rem(yy + d, 4) for d in range(4)]
    zs4 = [lax.rem(z + d, 4) for d in range(4)]

    def coords(sw):
        return lax.div(sw, 8), lax.rem(lax.div(sw, 2), 4), lax.rem(sw, 2)

    pairs = (
        (innov_hbm, innov), (prec_hbm, prec), (col_hbm, col), (chan_hbm, chan), (pred_hbm, pred),
        (smooth_hbm, smooth), (biasp_hbm, biasp), (jac_hbm, jac),
    )
    loads = [pltpu.make_async_copy(a, b, s_load.at[i]) for i, (a, b) in enumerate(pairs)]
    for cp in loads:
        cp.start()
    for ph in range(3):
        for r in (0, 1, 34, 35):
            gp[ph, r] = jnp.zeros((80, 128), f32)

    def chips(f):
        def hops(d):
            return sum(min(v, 4 - v) for v in (d // 16, d // 4 % 4, d % 4))

        for d in sorted(range(1, 64), key=hops, reverse=True):
            f((xs4[d // 16], ys4[d // 4 % 4], c, zs4[d % 4]))

    above, below = coords(s - 1), coords(s + 1)
    left, right = zs4[3], zs4[1]
    has_above, has_below = s > 0, s < 31

    barrier = pltpu.get_barrier_semaphore()

    def greet(to):
        pl.semaphore_signal(barrier, inc=1, device_id=to, device_id_type=MESH)

    chips(greet)
    for there, side in ((has_above, above), (has_below, below)):
        @pl.when(there)
        def _(side=side):
            for to_z in (z, left, right):
                greet(side + (to_z,))

    greeted = 63 + jnp.where(has_above, 3, 0) + jnp.where(has_below, 3, 0)

    for cp in loads[:7]:
        cp.wait()
    slot = lax.broadcasted_iota(i32, (LINES, 128), 0) * 128 + lax.broadcasted_iota(i32, (LINES, 128), 1)
    w[...] = jnp.where(slot < count[0, 0], prec[...], 0.0)
    y[...] = w[...] * innov[...]

    iota_s = lax.broadcasted_iota(i32, (128, 128), 0)
    iota_l = lax.broadcasted_iota(i32, (128, 128), 1)

    def count_of(m, v=1):
        return sum8(jnp.where(m, v, 0))

    a = jnp.broadcast_to(col[:, 0:1] >> 6, (128, 128))
    row_l = count_of(iota_s == iota_l, a)
    b = bc(row_l, 128)
    rank = jnp.transpose(bc(count_of((a < b) | ((a == b) & (iota_s < iota_l))), 128))
    put = rank == iota_l
    iv[0:1] = count_of(put, iota_s)
    iv[1:2] = count_of(put, a)
    iv[2:3] = jnp.maximum(count_of(a <= iota_l) - 1, 0)
    iv[3:4] = count_of(a == iota_l)
    iv[4:5] = row_l
    iv[5:8] = jnp.zeros((3, 128), i32)
    to_smem = pltpu.make_async_copy(iv, sm_i, s_load.at[8])
    to_smem.start()
    cl[...] = col[...] & 63

    for i in range(8):
        ob[i] = jnp.zeros((8, 128), f32)

    def pair_send(send, pair, ph):
        pltpu.make_async_remote_copy(
            src_ref=send.at[pl.ds(20 - half, 20)], dst_ref=pair, send_sem=s_pr_s.at[ph],
            recv_sem=s_pr_r.at[ph], device_id=partner, device_id_type=MESH,
        ).start()

    def scatter(send, pair, recv, ph):
        wait_all(pair, s_pr_r.at[ph])
        for i in range(20):
            pair[i] = pair[i] + send[half + i]
        for i in range(20):
            tz = zs4[i // 5]
            jj = lax.rem(x + yy + i % 5, 5)
            sw = 6 * jj + 3 * c
            tx, ty = lax.div(sw, 8), lax.rem(lax.div(sw, 2), 4)
            away = (tx != x) | (ty != yy) | (tz != z)

            @pl.when(away)
            def _(tz=tz, jj=jj, tx=tx, ty=ty):
                pltpu.make_async_remote_copy(
                    src_ref=pair.at[tz * 5 + jj], dst_ref=recv.at[chip], send_sem=s_rs_s.at[ph],
                    recv_sem=s_rs_r.at[ph], device_id=(tx, ty, c, tz), device_id_type=MESH,
                ).start()

        @pl.when(owner)
        def _():
            recv[chip] = pair[mine - half]

    def gathered(recv, ph):
        wait_all(recv.at[pl.ds(0, 63)], s_rs_r.at[ph])
        parts = [recv[i] for i in range(4)]
        for i in range(4, 64):
            parts[i % 4] += recv[i]
        return (parts[0] + parts[1]) + (parts[2] + parts[3])

    def spread(k):
        def send(to):
            pltpu.make_async_remote_copy(
                src_ref=zt.at[k, mine], dst_ref=zt.at[k, mine], send_sem=s_ag_s.at[k],
                recv_sem=s_ag_r.at[k], device_id=to, device_id_type=MESH,
            ).start()

        chips(send)

    def relay(k):
        ours = zt.at[k, pl.ds(half, 20)]
        return pltpu.make_async_remote_copy(
            src_ref=ours, dst_ref=ours, send_sem=s_rl_s.at[k], recv_sem=s_rl_r.at[k],
            device_id=partner, device_id_type=MESH,
        )

    def wait_spread(k):
        @pl.when(owner)
        def _():
            wait_all(zt.at[k, pl.ds(0, 19)], s_ag_r.at[k])

        @pl.when(jnp.logical_not(owner))
        def _():
            wait_all(zt.at[k, pl.ds(0, 20)], s_ag_r.at[k])

        relay(k).start()
        wait_all(zt.at[k, pl.ds(0, 20)], s_rl_r.at[k])

    lane = lax.broadcasted_iota(i32, (1, 128), 1)

    def scalar_pair(ph):
        return pltpu.make_async_remote_copy(
            src_ref=sp.at[ph, 0], dst_ref=sp.at[ph, 1], send_sem=s_sp_s.at[ph],
            recv_sem=s_sp_r.at[ph], device_id=partner, device_id_type=MESH,
        )

    def scalars_a(ph, rows):
        row = jnp.zeros((1, 128), f32)
        for i, r in enumerate(rows):
            row = jnp.where(lane == i, jnp.sum(r, axis=1, keepdims=True), row)
        sp[ph, 0] = row
        scalar_pair(ph).start()

    def scalars_b(ph):
        scalar_pair(ph).wait_recv()
        sc[ph, chip] = sp[ph, 0] + sp[ph, 1]

        def send(to):
            pltpu.make_async_remote_copy(
                src_ref=sc.at[ph, chip], dst_ref=sc.at[ph, chip], send_sem=s_sc_s.at[ph],
                recv_sem=s_sc_r.at[ph], device_id=to, device_id_type=MESH,
            ).start()

        chips(send)

    def scalars_c(ph):
        wait_all(sc.at[ph, pl.ds(0, 63)], s_sc_r.at[ph])
        parts = [sc[ph, i] for i in range(4)]
        for i in range(4, 64):
            parts[i % 4] += sc[ph, i]
        total = (parts[0] + parts[1]) + (parts[2] + parts[3])
        return tuple(jnp.broadcast_to(total[:, i : i + 1], (1, 128)) for i in range(3))

    def halo_copies(ph):
        def mk(n, src, dst, to):
            return pltpu.make_async_remote_copy(
                src_ref=src, dst_ref=dst, send_sem=s_halo_s.at[ph, n],
                recv_sem=s_halo_r.at[ph, n], device_id=to, device_id_type=MESH,
            )

        g = gp.at[ph]
        mid = pl.ds(8, LON)
        sides = [
            mk(0, est.at[ph, 0], hcol.at[ph, 1], (x, yy, c, left)),
            mk(1, est.at[ph, 1], hcol.at[ph, 0], (x, yy, c, right)),
        ]
        up = [
            mk(2, g.at[pl.ds(2, 2), mid], g.at[pl.ds(34, 2), mid], above + (z,)),
            mk(3, g.at[2, pl.ds(8, 8)], cn.at[ph, 0], above + (left,)),
            mk(4, g.at[2, pl.ds(64, 8)], cn.at[ph, 1], above + (right,)),
        ]
        down = [
            mk(5, g.at[pl.ds(32, 2), mid], g.at[pl.ds(0, 2), mid], below + (z,)),
            mk(6, g.at[33, pl.ds(8, 8)], cn.at[ph, 2], below + (left,)),
            mk(7, g.at[33, pl.ds(64, 8)], cn.at[ph, 3], below + (right,)),
        ]
        return sides, up, down

    def halo_send(ph):
        for r in range(LAT):
            g = jnp.where(sm_i[3, r] > 0, seg[sm_i[2, r]], 0.0)
            gp[ph, r + 2, 8:72, :] = g
            est[ph, 0, 2 * r : 2 * r + 2, :] = g[0:2]
            est[ph, 1, 2 * r : 2 * r + 2, :] = g[62:64]
        sides, up, down = halo_copies(ph)
        for cp in sides:
            cp.start()

        @pl.when(has_above)
        def _():
            for cp in up:
                cp.start()

        @pl.when(has_below)
        def _():
            for cp in down:
                cp.start()

    def halo_wait(ph):
        sides, up, down = halo_copies(ph)
        for cp in sides:
            cp.wait_recv()

        @pl.when(has_below)
        def _():
            for cp in up:
                cp.wait_recv()
            gp[ph, 34, 72:73, :] = cn[ph, 0, 0:1]
            gp[ph, 34, 7:8, :] = cn[ph, 1, 7:8]

        @pl.when(has_above)
        def _():
            for cp in down:
                cp.wait_recv()
            gp[ph, 1, 72:73, :] = cn[ph, 2, 0:1]
            gp[ph, 1, 7:8, :] = cn[ph, 3, 7:8]

        for r in range(LAT):
            gp[ph, r + 2, 72:74, :] = hcol[ph, 1, 2 * r : 2 * r + 2]
            gp[ph, r + 2, 6:8, :] = hcol[ph, 0, 2 * r : 2 * r + 2]

    def halo_done(ph):
        sides, up, down = halo_copies(ph)
        for cp in sides:
            cp.wait_send()

        @pl.when(has_above)
        def _():
            for cp in up:
                cp.wait_send()

        @pl.when(has_below)
        def _():
            for cp in down:
                cp.wait_send()

    sm = smooth[...]

    def smoothed(ref, r):
        v = ref[r]
        beside = ref[r - 1] + ref[r + 1] + pltpu.roll(v, 1, 0) + pltpu.roll(v, 79, 0)
        return v + sm * (beside - 4.0 * v)

    def inside(r):
        return ((r > 1) | has_above) & ((r < 34) | has_below)

    def squares(v):
        v = v * v
        t = v[0:8]
        for i in range(1, LON // 8):
            t += v[8 * i : 8 * i + 8]
        return t

    def to_forward(src):
        def step(r, total):
            u = smoothed(src, r)[8:72]
            hi, lo = split(u)
            u2[r - 2, 0:LON] = hi
            u2[r - 2, LON : 2 * LON] = lo
            return total + squares(src[r, 8:72, :])

        return sum8(lax.fori_loop(2, 34, step, jnp.zeros((8, 128), f32)))

    def slots_of(k):
        wait_spread(k)
        make_table(zt.at[k], tab)
        lookup(tab, oh, chan, pred, pc)
        image = hs[...] + pc[...]
        yw = w[...] * image
        y[...] = yw
        return sum8(yw * image)

    def term_y(b):
        return pred[:, lanes(b)] * y[pl.ds(b, 1), :]

    def term_d(b):
        p = pred[:, lanes(b)]
        return p * p * w[pl.ds(b, 1), :]

    bias_adjoint([term_y, term_d], chan, oh, lhs, acc, fill=True)
    for t in range(TILES):
        rs0_send[place(t), 0:8] = acc_tile(acc, 0, t)
        rs0_send[place(t), 8:16] = acc_tile(acc, 1, t)
    pl.semaphore_wait(barrier, greeted)
    pair_send(rs0_send, pr0, 0)
    to_smem.wait()
    loads[7].wait()
    scatter(rs0_send, pr0, rs0_recv, 0)
    adjoint(y, jac, sm_i, cl, seg)
    halo_send(0)

    @pl.when(owner)
    def _():
        both = gathered(rs0_recv, 0)
        bp = biasp[:, lanes(lax.div(s, 3))]
        rb, dg = both[0:8], both[8:16] + bp
        zb = rb / dg
        ob[0] = rb
        ob[1] = dg
        ob[2] = zb
        ob[3] = bp
        zt[0, mine] = zb
        spread(0)

    halo_wait(0)

    def first(r, _):
        r0[r] = jnp.where(inside(r), smoothed(gp.at[0], r), 0.0)
        return 0

    lax.fori_loop(1, 35, first, 0)
    rr_state = to_forward(r0)

    forward(u2, jac, sm_i, cl, hs)
    d0 = slots_of(0)
    scalars_a(0, (
        rr_state + sum8(ob[0] * ob[2]),
        rr_state + d0 + sum8(ob[3] * ob[2] * ob[2]),
        rr_state + sum8(ob[0] * ob[0]),
    ))
    bias_adjoint([term_y], chan, oh, lhs, acc)
    for t in range(TILES):
        rs_send[0, place(t)] = acc_tile(acc, 0, t)
    pair_send(rs_send.at[0], pr.at[0], 1)
    scatter(rs_send.at[0], pr.at[0], rs_recv.at[0], 1)
    scalars_b(0)
    adjoint(y, jac, sm_i, cl, seg)
    halo_send(1)
    rz0, pq0, rr0 = scalars_c(0)
    alpha0 = rz0 / pq0

    @pl.when(owner)
    def _():
        qb = ob[3] * ob[2] + gathered(rs_recv.at[0], 1)
        rb = ob[0] - alpha0 * qb
        zb = rb / ob[1]
        ob[4] = qb
        ob[5] = rb
        ob[6] = zb
        zt[1, mine] = zb
        spread(1)

    halo_wait(1)

    def second(r, _):
        q = r0[r] + jnp.where(inside(r), smoothed(gp.at[1], r), 0.0)
        q0[r] = q
        r1[r] = r0[r] - alpha0 * q
        return 0

    lax.fori_loop(1, 35, second, 0)
    rr_state = to_forward(r1)

    forward(u2, jac, sm_i, cl, hs)
    d1 = slots_of(1)
    scalars_a(1, (
        rr_state + sum8(ob[5] * ob[6]),
        rr_state + d1 + sum8(ob[3] * ob[6] * ob[6]),
        rr_state + sum8(ob[5] * ob[5]),
    ))
    bias_adjoint([term_y], chan, oh, lhs, acc)
    for t in range(TILES):
        rs_send[1, place(t)] = acc_tile(acc, 0, t)
    pair_send(rs_send.at[1], pr.at[1], 2)
    scatter(rs_send.at[1], pr.at[1], rs_recv.at[1], 2)
    scalars_b(1)
    adjoint(y, jac, sm_i, cl, seg)
    halo_send(2)
    rz1, zaz, rr1 = scalars_c(1)
    beta = rz1 / rz0
    alpha1 = rz1 / (zaz - beta * rz1 / alpha0)
    mix = alpha0 + alpha1 * beta

    def solved(r, _):
        xs[r - 2] = mix * r0[r, 8:72, :] + alpha1 * r1[r, 8:72, :]
        return 0

    lax.fori_loop(2, 34, solved, 0)
    store_x = pltpu.make_async_copy(xs, out_x, s_load.at[9])
    store_x.start()
    for t in range(10):
        at = (t % 2) * 20 + z * 5 + t // 2
        out_b[:, t * 128 : (t + 1) * 128] = mix * zt[0, at] + alpha1 * zt[1, at]

    @pl.when(owner)
    def _():
        qb = ob[3] * ob[6] + gathered(rs_recv.at[1], 2) + beta * ob[4]
        ob[7] = ob[5] - alpha1 * qb

    halo_wait(2)

    def last(r, total):
        v = r1[r, 8:72, :]
        q = v + smoothed(gp.at[2], r)[8:72] + beta * q0[r, 8:72, :]
        return total + squares(v - alpha1 * q)

    rr_state = sum8(lax.fori_loop(2, 34, last, jnp.zeros((8, 128), f32)))
    scalars_a(2, (rr_state + sum8(ob[7] * ob[7]),))
    scalars_b(2)
    rr2, _, _ = scalars_c(2)
    out_n[...] = jnp.sqrt(jnp.where(lane == 0, rr0, jnp.where(lane == 1, rr1, rr2)))

    for ph, ref in ((0, pr0), (1, pr.at[0]), (2, pr.at[1])):
        wait_all(ref, s_pr_s.at[ph])

        @pl.when(owner)
        def _(ph=ph, ref=ref):
            wait_all(ref.at[pl.ds(0, 19)], s_rs_s.at[ph])

        @pl.when(jnp.logical_not(owner))
        def _(ph=ph, ref=ref):
            wait_all(ref, s_rs_s.at[ph])

    @pl.when(owner)
    def _():
        for k in range(2):
            wait_all(rs_recv.at[0, pl.ds(0, 63)], s_ag_s.at[k])

    for k in range(2):
        relay(k).wait_send()
    for ph in range(3):
        halo_done(ph)
        scalar_pair(ph).wait_send()
        wait_all(sc.at[ph, pl.ds(0, 63)], s_sc_s.at[ph])
    store_x.wait()


def finish(x_in, b_in, n_in, x_out, b_out, n_out, hold, held_b, sem):
    first = pltpu.make_async_copy(b_in, held_b, sem.at[0])
    first.start()
    rows = LAT // PIECES
    come = []
    for i in range(PIECES):
        part = pl.ds(i * rows, rows)
        cp = pltpu.make_async_copy(x_in.at[part], hold.at[part], sem.at[2 + i])
        cp.start()
        come.append(cp)
    n_out[...] = n_in[:, 0:3]
    first.wait()
    second = pltpu.make_async_copy(held_b, b_out, sem.at[1])
    second.start()
    go = [second]
    for i, cp in enumerate(come):
        part = pl.ds(i * rows, rows)
        cp.wait()
        out = pltpu.make_async_copy(hold.at[part], x_out.at[part], sem.at[2 + PIECES + i])
        out.start()
        go.append(out)
    for cp in go:
        cp.wait()


def body(innovations, obs_precision, jacobian, predictors, obs_column, obs_channel, obs_count, smoothing, bias_precision):
    vm = pl.BlockSpec(memory_space=pltpu.VMEM)
    hbm = pl.BlockSpec(memory_space=pl.ANY)
    src = pl.BlockSpec(memory_space=pltpu.HBM)
    sq = (LINES, 128)
    V = pltpu.VMEM
    D = pltpu.SemaphoreType.DMA
    out = pl.pallas_call(
        kernel,
        name="pcg",
        out_shape=(
            jax.ShapeDtypeStruct((LAT, LON, LEV), f32),
            jax.ShapeDtypeStruct((NPRED, 1280), f32),
            jax.ShapeDtypeStruct((1, 128), f32),
        ),
        in_specs=[src] * 6 + [pl.BlockSpec(memory_space=pltpu.SMEM), src, src],
        out_specs=(hbm, vm, vm),
        scratch_shapes=[
            V(sq, f32), V(sq, f32), V((NPRED, 16384), f32), V(sq, i32), V(sq, i32), V((1, LEV), f32), V((NPRED, 1280), f32),
            V((LINES, 128, LEV), bf16), V((LINES, 256, 128), bf16), V((KL, 640, 128), bf16), V((640, 256), f32), V((320, 256), bf16),
            V(sq, f32), V(sq, f32), V(sq, f32), V(sq, f32),
            V((LAT, 2 * LON, LEV), bf16), V((LINES, LON, LEV), f32),
            V((3, 36, 80, LEV), f32), V((36, 80, LEV), f32), V((36, 80, LEV), f32), V((36, 80, LEV), f32),
            V((LAT, LON, LEV), f32), V((3, 2, 64, LEV), f32), V((3, 2, 64, LEV), f32), V((3, 4, 8, LEV), f32),
            V((TILES, 16, 128), f32), V((20, 16, 128), f32), V((64, 16, 128), f32),
            V((2, TILES, 8, 128), f32), V((2, 20, 8, 128), f32), V((2, 64, 8, 128), f32),
            V((2, TILES, 8, 128), f32), V((3, 2, 1, 128), f32), V((3, 64, 1, 128), f32), V((8, 8, 128), f32),
            V((8, 128), i32), V(sq, i32), pltpu.SMEM((8, 128), i32),
            D((10,)), D((3, 8)), D((3, 8)), D((3,)), D((3,)), D((3,)), D((3,)), D((2,)), D((2,)), D((2,)), D((2,)),
            D((3,)), D((3,)), D((3,)), D((3,)),
        ],
        compiler_params=pltpu.CompilerParams(
            collective_id=0, has_side_effects=True, vmem_limit_bytes=62 * 2**20
        ),
    )(
        innovations.reshape(sq), obs_precision.reshape(sq), jacobian.reshape(LINES, 128, LEV), predictors,
        obs_column.reshape(sq), obs_channel.reshape(sq), obs_count, smoothing.reshape(1, LEV), bias_precision,
    )
    done = pl.pallas_call(
        finish,
        name="finish",
        out_shape=(
            jax.ShapeDtypeStruct((LAT, LON, LEV), f32),
            jax.ShapeDtypeStruct((NPRED, 1280), f32),
            jax.ShapeDtypeStruct((1, 3), f32),
        ),
        in_specs=[hbm, hbm, vm],
        out_specs=(hbm, hbm, vm),
        scratch_shapes=[V((LAT, LON, LEV), f32), V((NPRED, 1280), f32), D((2 + 2 * PIECES,))],
        compiler_params=pltpu.CompilerParams(vmem_limit_bytes=62 * 2**20),
    )(*out)
    return done[0], done[1], done[2][0]


def solution(mesh):
    torus = Mesh(mesh.devices.reshape(4, 4, 2, mesh.shape["chan"]), AX)
    placed = (
        P(AX), P(AX), P(AX, None), P(None, AX), P(AX), P(AX), P(SWATH, "chan"), P(), P(None, "chan"),
    )
    return jax.shard_map(
        body,
        mesh=torus,
        in_specs=placed,
        out_specs=(P(SWATH, "chan", None), P(None, "chan"), P()),
        check_vma=False,
    )
```
